16 devices in a mesh: ez: 2 (over z), ey: 2 (over y), ex: 4 (over x, core).
Axes of the slice: x: 2, y: 2, z: 2, core: 2. Of those that a mesh axis runs over, the one named last changes fastest.
Arguments:
- x_tokens: bfloat16 [8192, 2048], P(('ez', 'ey', 'ex'))
- expert_ids: int32 [8192, 6], P(('ez', 'ey', 'ex'))
- gate_vals: float32 [8192, 6], P(('ez', 'ey', 'ex'))
- w_gate: bfloat16 [64, 2048, 1408], P(('ex', 'ey', 'ez'))
- w_up: bfloat16 [64, 2048, 1408], P(('ex', 'ey', 'ez'))
- w_down: bfloat16 [64, 1408, 2048], P(('ex', 'ey', 'ez'))
Outputs:
- output: bfloat16 [8192, 2048], P(('ez', 'ey', 'ex'))
All inputs are finite; a program needn't handle non-finite values.
Results may differ from the reference program's by a relative error of at most 0.00115.
Values are sent between devices in bfloat16 or wider.
A program may use at most 1 GiB of HBM per device.

```python
import jax
import jax.numpy as jnp
from jax import lax

HIDDEN = 2048
FFN_DIM = 1408
EXPERTS = 64
TOP_K = 6
TOK_DEV = 512
DEVICES = 16
GROUPS = 8

TOKENS_ALL = DEVICES * TOK_DEV
CAP_EXPERT = 2 * DEVICES * TOK_DEV * TOP_K // EXPERTS


def draw_routing(route_key):
    perm_key, group_key = jax.random.split(route_key)
    group_size = EXPERTS // GROUPS
    pair_count = group_size // 2
    pick_groups = TOP_K // 2
    perm_score = jax.random.randint(perm_key, (DEVICES, GROUPS, group_size), 0, 1 << 20)
    inner_perm = jnp.argsort(perm_score * group_size + jnp.arange(group_size), axis=-1)
    inner_perm = inner_perm.at[:, :, 2].set(inner_perm[:, :, 0])
    group_score = jax.random.randint(group_key, (DEVICES, GROUPS), 0, 1 << 20)
    group_perm = jnp.argsort(group_score * GROUPS + jnp.arange(GROUPS), axis=-1)
    visit_idx = jnp.arange(TOK_DEV)[:, None] * pick_groups + jnp.arange(pick_groups)[None, :]
    dev_idx = jnp.arange(DEVICES)[:, None, None]
    group_id = group_perm[dev_idx, visit_idx[None] % GROUPS]
    pair_pos = 2 * ((visit_idx // GROUPS) % pair_count)[None]
    first_pick = inner_perm[dev_idx, group_id, pair_pos]
    second_pick = inner_perm[dev_idx, group_id, pair_pos + 1]
    local_pick = jnp.stack([first_pick, second_pick], axis=-1)
    expert_ids = group_id[:, :, :, None] * group_size + local_pick
    return expert_ids.reshape(TOKENS_ALL, TOP_K).astype(jnp.int32)


def setup_inputs(seed: int = 0) -> dict:
    base_key = jax.random.key(seed)
    key_x, key_gate, key_one, key_three, key_two, key_route = jax.random.split(base_key, 6)
    x_tokens = jax.random.normal(key_x, (TOKENS_ALL, HIDDEN), jnp.float32)
    gate_raw = jax.random.uniform(key_gate, (TOKENS_ALL, TOP_K), jnp.float32, 0.5, 1.5)
    gate_vals = 2.5 * gate_raw / jnp.sum(gate_raw, axis=1, keepdims=True)
    w_gate = jax.random.normal(key_one, (EXPERTS, HIDDEN, FFN_DIM), jnp.float32) * HIDDEN ** -0.5
    w_up = jax.random.normal(key_three, (EXPERTS, HIDDEN, FFN_DIM), jnp.float32) * HIDDEN ** -0.5
    w_down = jax.random.normal(key_two, (EXPERTS, FFN_DIM, HIDDEN), jnp.float32) * FFN_DIM ** -0.5
    return {
        'x_tokens': x_tokens.astype(jnp.bfloat16),
        'expert_ids': draw_routing(key_route),
        'gate_vals': gate_vals,
        'w_gate': w_gate.astype(jnp.bfloat16),
        'w_up': w_up.astype(jnp.bfloat16),
        'w_down': w_down.astype(jnp.bfloat16),
    }


def reference(x_tokens, expert_ids, gate_vals, w_gate, w_up, w_down):
    flat_ids = expert_ids.reshape(-1)
    flat_gates = gate_vals.reshape(-1)
    pair_tok = jnp.arange(TOKENS_ALL * TOP_K) // TOP_K
    slot_pos = jnp.arange(CAP_EXPERT)

    def expert_step(acc_sum, scan_in):
        expert, w_one, w_three, w_two = scan_in
        chosen = flat_ids == expert
        n_chosen = jnp.sum(chosen.astype(jnp.int32))
        pair_sel = jnp.nonzero(chosen, size=CAP_EXPERT, fill_value=0)[0]
        tok_sel = pair_tok[pair_sel]
        weight = jnp.where(slot_pos < n_chosen, flat_gates[pair_sel], 0.0)
        tok_rows = x_tokens[tok_sel]
        h_gate = jnp.dot(tok_rows, w_one, preferred_element_type=jnp.float32)
        h_up = jnp.dot(tok_rows, w_three, preferred_element_type=jnp.float32)
        act_bf = (jax.nn.silu(h_gate) * h_up).astype(jnp.bfloat16)
        exp_out = jnp.dot(act_bf, w_two, preferred_element_type=jnp.float32).astype(jnp.bfloat16)
        acc_sum = acc_sum.at[tok_sel].add(weight[:, None] * exp_out.astype(jnp.float32))
        return acc_sum, None

    acc_init = jnp.zeros((TOKENS_ALL, HIDDEN), jnp.float32)
    moe_sum = lax.scan(expert_step, acc_init, (jnp.arange(EXPERTS), w_gate, w_up, w_down))[0]
    return (x_tokens.astype(jnp.float32) + moe_sum).astype(jnp.bfloat16)
```

```python
import jax
import jax.numpy as jnp
from jax import lax
from jax.sharding import PartitionSpec as P

TOKEN_AXES = ('ez', 'ey', 'ex')
EXPERT_AXES = ('ex', 'ey', 'ez')


def routing(ids, gates, n_exp):
    tok_dev = ids.shape[0]
    hit = ids[:, :, None] == jnp.arange(n_exp)[None, None, :]
    picked = jnp.any(hit, axis=1)
    gate = jnp.sum(jnp.where(hit, gates[:, :, None], 0.0), axis=1)
    below = (jnp.arange(tok_dev)[:, None] > jnp.arange(tok_dev)[None, :]).astype(jnp.bfloat16)
    rank = jnp.dot(below, picked.astype(jnp.bfloat16), preferred_element_type=jnp.float32)
    return hit, picked, rank, gate


def solution(mesh):
    n_dev = mesh.shape['ez'] * mesh.shape['ey'] * mesh.shape['ex']

    def local_layer(x_loc, ids_loc, gates_loc, w_g, w_u, w_d):
        tok_dev, hid = x_loc.shape
        top_k = ids_loc.shape[1]
        n_local = w_g.shape[0]
        n_exp = n_local * n_dev
        cap = 2 * tok_dev * top_k // n_exp
        x_all = lax.all_gather(x_loc, TOKEN_AXES, tiled=True)
        hit, picked, rank, gate = routing(ids_loc, gates_loc, n_exp)
        code = jnp.where(picked, rank, -1.0).T.reshape(n_dev, n_local, tok_dev)
        code = lax.all_to_all(code, EXPERT_AXES, 0, 0)
        slot = jnp.arange(cap, dtype=jnp.float32)
        match = code[:, :, None, :] == slot[None, None, :, None]
        slot_tok = jnp.sum(jnp.where(match, jnp.arange(tok_dev, dtype=jnp.int32), 0), axis=-1)
        nz, ny, nx = mesh.shape['ez'], mesh.shape['ey'], mesh.shape['ex']
        num = jnp.arange(n_dev)
        tok_num = ((num % nz) * ny + (num // nz) % ny) * nx + num // (nz * ny)
        rows = (tok_num[:, None, None] * tok_dev + slot_tok)
        rows = rows.transpose(1, 0, 2).reshape(-1)
        xs = jnp.take(x_all, rows, axis=0, mode='clip').reshape(n_local, n_dev * cap, hid)
        h_gate = jnp.einsum('lch,lhf->lcf', xs, w_g, preferred_element_type=jnp.float32)
        h_up = jnp.einsum('lch,lhf->lcf', xs, w_u, preferred_element_type=jnp.float32)
        act = (jax.nn.silu(h_gate) * h_up).astype(jnp.bfloat16)
        out = jnp.einsum('lcf,lfh->lch', act, w_d, preferred_element_type=jnp.float32).astype(jnp.bfloat16)
        out = out.reshape(n_local, n_dev, cap, hid)
        back = lax.all_to_all(out, EXPERT_AXES, 1, 1)
        back = back.reshape(n_local * n_dev * cap, hid)
        rank_j = jnp.sum(jnp.where(hit, rank[:, None, :], 0.0), axis=-1).astype(jnp.int32)
        slot_idx = ((ids_loc % n_local) * n_dev + ids_loc // n_local) * cap + rank_j
        acc = x_loc.astype(jnp.float32)
        tok_rows = jnp.take(back, slot_idx.reshape(-1), axis=0, mode='clip').reshape(tok_dev, top_k, hid)
        acc = acc + jnp.sum(gates_loc[:, :, None] * tok_rows, axis=1)
        return acc.astype(jnp.bfloat16)

    tok = P(TOKEN_AXES, None)
    w = P(EXPERT_AXES, None, None)
    return jax.shard_map(local_layer, mesh=mesh, in_specs=(tok, tok, tok, w, w, w), out_specs=tok, check_vma=False)
```

```python
import functools

import jax
import jax.numpy as jnp
from jax import lax
from jax.experimental import pallas as pl
from jax.experimental.pallas import tpu as pltpu
from jax.sharding import PartitionSpec as P

TOKEN_AXES = ('ez', 'ey', 'ex')
EXPERT_AXES = ('ex', 'ey', 'ez')
MESH = pl.DeviceIdType.MESH
BF16, F32 = jnp.bfloat16, jnp.float32

N_DEV = 16
N_LOC = 4
N_EXP = N_DEV * N_LOC
TOK = 512
HID = 2048
FFN = 1408
CAP = 96
RET = 240
SLOTS = N_LOC * CAP
UNITS = (1, 3, 3, 1)
FIRST = (0, 1, 4, 7)


def routing(ids, gates):
    hit = ids[:, :, None] == jnp.arange(N_EXP)[None, None, :]
    picked = jnp.any(hit, axis=1)
    gate = jnp.sum(jnp.where(hit, gates[:, :, None], 0.0), axis=1)
    below = (jnp.arange(TOK)[:, None] > jnp.arange(TOK)[None, :]).astype(BF16)
    rank = jnp.dot(below, picked.astype(BF16), preferred_element_type=F32)
    return hit, picked, rank, gate


def tables(ids, gates):
    hit, picked, rank, gate = routing(ids, gates)
    cnt = jnp.sum(picked.astype(F32), axis=0).reshape(N_DEV, N_LOC)
    tri = (jnp.arange(N_LOC)[:, None] > jnp.arange(N_LOC)[None, :]).astype(F32)
    off = jnp.sum(cnt[:, None, :] * tri[None], axis=-1)
    over = jnp.max(jnp.sum(cnt, axis=1)) > RET
    code = jnp.where(picked, rank, -1.0).T.reshape(N_DEV, N_LOC, TOK)
    slot = jnp.arange(CAP, dtype=F32)
    pos = jnp.where(slot < cnt[:, :, None], off[:, :, None] + slot, -1.0).reshape(N_DEV, 1, SLOTS)
    pos = jnp.pad(pos, ((0, 0), (0, 0), (0, TOK - SLOTS)), constant_values=-1.0)
    flag = jnp.broadcast_to(over.astype(F32), (N_DEV, 3, TOK))
    codes = jnp.concatenate([code, pos, flag], axis=1)
    place = jnp.where(picked, off.reshape(-1)[None] + rank, -1.0)
    comb = jnp.concatenate([place, gate], axis=1)
    return codes, comb


def flips(q):
    ct, i = (q + 2) // 3, (q + 2) % 3
    w1, w2, w3 = (ct % 2) * (1 - ct // 2), (1 - ct % 2) * (ct // 2), (ct % 2) * (ct // 2)
    base = ((3 - i) // 3, i % 2, i // 2)
    return tuple(w1 * f + w2 * (1 - f) + w3 for f in base)


def moe_kernel(x_ref, codes_ref, comb_ref, w1_ref, w3_ref, w2_ref,
               y_ref, flag_ref, x_all, h_send, h_recv,
               wb1, wb3, wb2, rows, act, xb, sb, meta, acc,
               w_sem, xl_sem, xs_sem, xr_sem, ms_sem, mr_sem, sl_sem, rs_sem, rr_sem, rl_sem):
    ez, ey, ex = (lax.axis_index(a) for a in TOKEN_AXES)
    core, xc = ex % 2, ex // 2
    my_tok = (ez * 2 + ey) * 4 + ex
    my_exp = (ex * 2 + ey) * 2 + ez

    def place(q, other):
        cs = core + other * (1 - 2 * core)
        fa, fb, fc = flips(q)
        fx = fa * (1 - cs) + fb * cs
        fy = fb * (1 - cs) + fc * cs
        fz = fc * (1 - cs) + fa * cs
        pz, py, px = ez + fz * (1 - 2 * ez), ey + fy * (1 - 2 * ey), xc + fx * (1 - 2 * xc)
        return pz, py, 2 * px + cs

    def tok_num(p):
        return (p[0] * 2 + p[1]) * 4 + p[2]

    def exp_num(p):
        return (p[2] * 2 + p[1]) * 2 + p[0]

    barrier = pltpu.get_barrier_semaphore()

    @pl.loop(1, N_DEV)
    def _(d):
        pl.semaphore_signal(barrier, inc=1, device_id=place(d // 2, d % 2), device_id_type=MESH)

    pl.semaphore_wait(barrier, N_DEV - 1)

    def x_copy(src, slot, n, dev):
        return pltpu.make_async_remote_copy(
            src_ref=src, dst_ref=x_all.at[slot], send_sem=xs_sem.at[n], recv_sem=xr_sem.at[slot],
            device_id=dev, device_id_type=MESH)

    sib = place(0, 1)
    nbr = {1: place(1, 0), 2: place(2, 0), 3: place(3, 0)}
    for n, q in enumerate((1, 2, 3)):
        x_copy(x_ref, q, n, nbr[q]).start()
    x_copy(x_ref, 8, 3, sib).start()

    def forward(q, via, to, n):
        x_copy(x_all.at[q], to, n, nbr[via]).start()

    def push(q):
        x_copy(x_all.at[q], 8 + q, 3 + q, sib).start()

    def arrived(slot):
        x_copy(x_ref, slot, 0, sib).wait_recv()

    def meta_copy(d):
        dev = place(d // 2, d % 2)
        return pltpu.make_async_remote_copy(
            src_ref=codes_ref.at[exp_num(dev)], dst_ref=meta.at[my_tok], send_sem=ms_sem.at[d],
            recv_sem=mr_sem.at[my_tok], device_id=dev, device_id_type=MESH)

    own_meta = pltpu.make_async_copy(codes_ref.at[my_exp], meta.at[my_tok], mr_sem.at[my_tok])
    own_meta.start()

    @pl.loop(1, N_DEV)
    def _(d):
        meta_copy(d).start()

    def meta_wait(num):
        pltpu.make_async_copy(codes_ref.at[0], meta.at[num], mr_sem.at[num]).wait()

    def w_copies(e, s):
        return [pltpu.make_async_copy(w.at[e], b.at[s], w_sem.at[s, k])
                for k, (w, b) in enumerate(((w1_ref, wb1), (w3_ref, wb3), (w2_ref, wb2)))]

    for c in w_copies(0, 0):
        c.start()

    def gather(ci):
        n, q0 = 2 * UNITS[ci], FIRST[ci]

        def load(d):
            slot = q0 + d // 2 + 8 * (d % 2)
            return pltpu.make_async_copy(x_all.at[slot], xb.at[d % 2], xl_sem.at[d % 2])

        def fetch(d):
            arrived(q0 + d // 2 + 8 * (d % 2))
            load(d).start()

        if ci == 0:
            pltpu.make_async_copy(x_ref, xb.at[0], xl_sem.at[0]).start()
        else:
            load(0).start()

        @pl.loop(0, n)
        def _(d):
            @pl.when(d + 1 < n)
            def _():
                if ci == 0:
                    fetch(d + 1)
                else:
                    @pl.when((d + 1) % 2 == 1)
                    def _():
                        arrived(q0 + (d + 1) // 2 + 8)
                    load(d + 1).start()
            dev = place(q0 + d // 2, d % 2)
            num = tok_num(dev)
            meta_wait(num)
            code = meta[num]
            want = lax.broadcasted_iota(jnp.int32, (CAP, TOK), 0).astype(F32)
            sel = jnp.concatenate(
                [jnp.where(code[e:e + 1, :] == want, 1.0, 0.0).astype(BF16) for e in range(N_LOC)], axis=0)
            load(d).wait()
            at = pl.multiple_of(d * CAP, CAP)

            @pl.loop(0, HID // 512)
            def _(t):
                cols = pl.ds(pl.multiple_of(t * 512, 512), 512)
                got = jnp.dot(sel, xb[d % 2, :, cols], preferred_element_type=F32).astype(BF16)
                for e in range(N_LOC):
                    rows[e, pl.ds(at, CAP), cols] = got[e * CAP:(e + 1) * CAP]

    def ffn(ci, e):
        m = UNITS[ci] * 2 * CAP
        s = e % 2
        for c in w_copies(e, s):
            c.wait()
        def prefetch():
            for c in w_copies((e + 1) % N_LOC, 1 - s):
                c.start()
        if ci < 3:
            prefetch()
        else:
            pl.when(e + 1 < N_LOC)(prefetch)

        @pl.loop(0, FFN // 128)
        def _(t):
            cols = pl.ds(pl.multiple_of(t * 128, 128), 128)
            w = jnp.concatenate([wb1[s, :, cols], wb3[s, :, cols]], axis=1)
            h = jnp.dot(rows[e, :m, :], w, preferred_element_type=F32)
            act[:m, cols] = (jax.nn.silu(h[:, :128]) * h[:, 128:]).astype(BF16)

        @pl.loop(0, HID // 512)
        def _(t):
            cols = pl.ds(pl.multiple_of(t * 512, 512), 512)
            rows[e, :m, cols] = jnp.dot(act[:m, :], wb2[s, :, cols], preferred_element_type=F32).astype(BF16)

    def ret_copy(d):
        dev = place(d // 2, d % 2)
        return pltpu.make_async_remote_copy(
            src_ref=h_send.at[d], dst_ref=h_recv.at[my_exp], send_sem=rs_sem.at[d],
            recv_sem=rr_sem.at[my_exp], device_id=dev, device_id_type=MESH)

    def stage(d):
        return pltpu.make_async_copy(sb.at[d % 2], h_send.at[d], sl_sem.at[d % 2])

    def send_back(ci):
        d0, n = 2 * FIRST[ci], 2 * UNITS[ci]

        @pl.loop(0, n)
        def _(k):
            d = d0 + k
            num = tok_num(place(d // 2, d % 2))
            pos = meta[num, 4:5, :SLOTS]
            want = lax.broadcasted_iota(jnp.int32, (RET, SLOTS), 0).astype(F32)
            sel = jnp.where(pos == want, 1.0, 0.0).astype(BF16)
            at = pl.multiple_of(k * CAP, CAP)

            @pl.loop(0, HID // 512)
            def _(t):
                cols = pl.ds(pl.multiple_of(t * 512, 512), 512)
                o = jnp.concatenate([rows[e, pl.ds(at, CAP), cols] for e in range(N_LOC)], axis=0)
                sb[d % 2, :, cols] = jnp.dot(sel, o, preferred_element_type=F32).astype(BF16)

            stage(d).start()

            @pl.when(k > 0)
            def _():
                stage(d - 1).wait()
                if ci == 0:
                    pass
                else:
                    ret_copy(d - 1).start()

        last = d0 + n - 1
        stage(last).wait()
        ret_copy(last).start()

    def experts(ci, between=None):
        @pl.loop(0, N_LOC)
        def _(e):
            ffn(ci, e)
            if between is not None:
                pl.when(e == 2)(between)

    gather(0)
    experts(0)
    send_back(0)
    for q in (1, 2, 3):
        arrived(q)
        if q == 1:
            forward(1, 3, 5, 11)
        elif q == 2:
            forward(2, 1, 6, 12)
        else:
            forward(3, 2, 4, 13)
    for q in (1, 2, 3):
        push(q)
    gather(1)

    def relay():
        arrived(4)
        forward(4, 1, 7, 14)
        push(4)
        for q in (5, 6):
            arrived(q)
            push(q)

    experts(1, relay)
    send_back(1)
    gather(2)

    def relay_last():
        arrived(7)
        push(7)

    experts(2, relay_last)
    send_back(2)
    gather(3)
    experts(3)
    send_back(3)

    acc[...] = x_to_f32(x_ref, xb, xl_sem, acc)

    def take(d):
        num = exp_num(place(d // 2, d % 2))
        return pltpu.make_async_copy(h_recv.at[num], sb.at[d % 2], rl_sem.at[d % 2])

    def came(d):
        num = exp_num(place(d // 2, d % 2))
        pltpu.make_async_remote_copy(
            src_ref=h_send.at[d], dst_ref=h_recv.at[num], send_sem=rs_sem.at[d],
            recv_sem=rr_sem.at[num], device_id=sib, device_id_type=MESH).wait_recv()

    pltpu.make_async_copy(h_send.at[0], sb.at[0], rl_sem.at[0]).start()

    @pl.loop(0, N_DEV)
    def _(d):
        @pl.when(d + 1 < N_DEV)
        def _():
            came(d + 1)
            take(d + 1).start()
        num = exp_num(place(d // 2, d % 2))
        tab = pltpu.roll(comb_ref[...], (2 * N_EXP - num * N_LOC) % (2 * N_EXP), 1)
        want = lax.broadcasted_iota(jnp.int32, (TOK, RET), 1).astype(F32)
        g = jnp.zeros((TOK, RET), F32)
        for e in range(N_LOC):
            g = jnp.where(tab[:, e:e + 1] == want, tab[:, N_EXP + e:N_EXP + e + 1], g)
        hi = g.astype(BF16)
        rest = g - hi.astype(F32)
        mid = rest.astype(BF16)
        lo = (rest - mid.astype(F32)).astype(BF16)
        lhs = jnp.concatenate([hi, mid, lo], axis=0)
        take(d).wait()

        @pl.loop(0, HID // 256)
        def _(t):
            cols = pl.ds(pl.multiple_of(t * 256, 256), 256)
            r = jnp.dot(lhs, sb[d % 2, :, cols], preferred_element_type=F32)
            acc[:, cols] += r[:TOK] + (r[TOK:2 * TOK] + r[2 * TOK:])

    y_ref[...] = acc[...].astype(BF16)
    flag_ref[...] = jnp.max(meta[:, 5:6, :128], axis=0) + jnp.zeros((8, 128), F32)

    for n in range(15):
        x_copy(x_ref, 0, n, sib).wait_send()

    @pl.loop(1, N_DEV)
    def _(d):
        meta_copy(d).wait_send()
        ret_copy(d).wait_send()


def x_to_f32(x_ref, xb, xl_sem, acc):
    c = pltpu.make_async_copy(x_ref, xb.at[0], xl_sem.at[0])
    c.start()
    c.wait()
    return xb[0].astype(F32)


def moe(x, codes, comb, w1, w3, w2):
    hbm = pl.BlockSpec(memory_space=pl.ANY)
    vmem = pl.BlockSpec(memory_space=pltpu.VMEM)
    dma = pltpu.SemaphoreType.DMA
    out = pl.pallas_call(
        moe_kernel,
        out_shape=(
            jax.ShapeDtypeStruct((TOK, HID), BF16),
            jax.ShapeDtypeStruct((8, 128), F32),
            jax.ShapeDtypeStruct((N_DEV, TOK, HID), BF16),
            jax.ShapeDtypeStruct((N_DEV, RET, HID), BF16),
            jax.ShapeDtypeStruct((N_DEV, RET, HID), BF16),
        ),
        in_specs=[hbm, hbm, vmem, hbm, hbm, hbm],
        out_specs=(vmem, vmem, hbm, hbm, hbm),
        scratch_shapes=[
            pltpu.VMEM((2, HID, FFN), BF16),
            pltpu.VMEM((2, HID, FFN), BF16),
            pltpu.VMEM((2, FFN, HID), BF16),
            pltpu.VMEM((N_LOC, 6 * CAP, HID), BF16),
            pltpu.VMEM((6 * CAP, FFN), BF16),
            pltpu.VMEM((2, TOK, HID), BF16),
            pltpu.VMEM((2, RET, HID), BF16),
            pltpu.VMEM((N_DEV, 8, TOK), F32),
            pltpu.VMEM((TOK, HID), F32),
            dma((2, 3)), dma((2,)), dma((15,)), dma((16,)), dma((16,)), dma((16,)),
            dma((2,)), dma((16,)), dma((16,)), dma((2,)),
        ],
        compiler_params=pltpu.CompilerParams(
            collective_id=0, has_side_effects=True, vmem_limit_bytes=67_043_328),
        name='moe',
    )(x, codes, comb, w1, w3, w2)
    return out[0], out[1]


def plain(x_loc, ids, gates, w_g, w_u, w_d):
    hit, picked, rank, gate = routing(ids, gates)
    code = jnp.where(picked, rank, -1.0).T.reshape(N_DEV, N_LOC, TOK)
    match = code[:, :, None, :] == jnp.arange(CAP, dtype=F32)[None, None, :, None]
    slot_tok = jnp.sum(jnp.where(match, jnp.arange(TOK, dtype=jnp.int32), 0), axis=-1)
    send = jnp.take(x_loc, slot_tok.reshape(-1), axis=0, mode='clip').reshape(N_DEV, N_LOC, CAP, HID)
    recv = lax.all_to_all(send, EXPERT_AXES, 0, 0)
    h_gate = jnp.einsum('slch,lhf->slcf', recv, w_g, preferred_element_type=F32)
    h_up = jnp.einsum('slch,lhf->slcf', recv, w_u, preferred_element_type=F32)
    act = (jax.nn.silu(h_gate) * h_up).astype(BF16)
    out = jnp.einsum('slcf,lfh->slch', act, w_d, preferred_element_type=F32).astype(BF16)
    back = lax.all_to_all(out, EXPERT_AXES, 0, 0).reshape(N_EXP * CAP, HID)
    rank_j = jnp.sum(jnp.where(hit, rank[:, None, :], 0.0), axis=-1).astype(jnp.int32)
    got = jnp.take(back, (ids * CAP + rank_j).reshape(-1), axis=0, mode='clip').reshape(TOK, -1, HID)
    return (x_loc.astype(F32) + jnp.sum(gates[:, :, None] * got, axis=1)).astype(BF16)


def solution(mesh):
    def local_layer(x, ids, gates, w1, w3, w2):
        codes, comb = tables(ids, gates)
        y, flag = moe(x, codes, comb, w1, w3, w2)
        return lax.cond(flag[0, 0] > 0.0, lambda: plain(x, ids, gates, w1, w3, w2), lambda: y)

    tok = P(TOKEN_AXES, None)
    w = P(EXPERT_AXES, None, None)
    return jax.shard_map(local_layer, mesh=mesh, in_specs=(tok, tok, tok, w, w, w), out_specs=tok, check_vma=False)
```

```python
import functools

import jax
import jax.numpy as jnp
from jax import lax
from jax.experimental import pallas as pl
from jax.experimental.pallas import tpu as pltpu
from jax.sharding import PartitionSpec as P

TOKEN_AXES = ('ez', 'ey', 'ex')
EXPERT_AXES = ('ex', 'ey', 'ez')
MESH = pl.DeviceIdType.MESH
BF16, F32 = jnp.bfloat16, jnp.float32

N_DEV = 16
N_LOC = 4
N_EXP = N_DEV * N_LOC
TOK = 512
HID = 2048
FFN = 1408
CAP = 96
RET = 240
SLOTS = N_LOC * CAP
UNITS = (1, 3, 3, 1)
FIRST = (0, 1, 4, 7)


def routing(ids, gates):
    hit = ids[:, :, None] == jnp.arange(N_EXP)[None, None, :]
    picked = jnp.any(hit, axis=1)
    gate = jnp.sum(jnp.where(hit, gates[:, :, None], 0.0), axis=1)
    below = (jnp.arange(TOK)[:, None] > jnp.arange(TOK)[None, :]).astype(BF16)
    rank = jnp.dot(below, picked.astype(BF16), preferred_element_type=F32)
    return hit, picked, rank, gate


def tables(ids, gates):
    hit, picked, rank, gate = routing(ids, gates)
    cnt = jnp.sum(picked.astype(F32), axis=0).reshape(N_DEV, N_LOC)
    tri = (jnp.arange(N_LOC)[:, None] > jnp.arange(N_LOC)[None, :]).astype(F32)
    off = jnp.sum(cnt[:, None, :] * tri[None], axis=-1)
    over = jnp.max(jnp.sum(cnt, axis=1)) > RET
    code = jnp.where(picked, rank, -1.0).T.reshape(N_DEV, N_LOC, TOK)
    slot = jnp.arange(CAP, dtype=F32)
    pos = jnp.where(slot < cnt[:, :, None], off[:, :, None] + slot, -1.0).reshape(N_DEV, 1, SLOTS)
    pos = jnp.pad(pos, ((0, 0), (0, 0), (0, TOK - SLOTS)), constant_values=-1.0)
    flag = jnp.broadcast_to(over.astype(F32), (N_DEV, 3, TOK))
    codes = jnp.concatenate([code, pos, flag], axis=1)
    place = jnp.where(picked, off.reshape(-1)[None] + rank, -1.0)
    comb = jnp.concatenate([place, gate], axis=1)
    return codes, comb


def flips(q):
    ct, i = (q + 2) // 3, (q + 2) % 3
    w1, w2, w3 = (ct % 2) * (1 - ct // 2), (1 - ct % 2) * (ct // 2), (ct % 2) * (ct // 2)
    base = ((3 - i) // 3, i % 2, i // 2)
    return tuple(w1 * f + w2 * (1 - f) + w3 for f in base)


def moe_kernel(x_ref, codes_ref, comb_ref, w1_ref, w3_ref, w2_ref,
               y_ref, flag_ref, x_all, h_send, h_recv, h_pass,
               wb1, wb3, wb2, rows, act, xb, sb, meta, acc,
               w_sem, xl_sem, xs_sem, xr_sem, ms_sem, mr_sem, sl_sem, rs_sem, rr_sem, rl_sem, ps_sem, pr_sem):
    ez, ey, ex = (lax.axis_index(a) for a in TOKEN_AXES)
    core, xc = ex % 2, ex // 2
    my_tok = (ez * 2 + ey) * 4 + ex
    my_exp = (ex * 2 + ey) * 2 + ez

    def place(q, other):
        cs = core + other * (1 - 2 * core)
        return moved(q, cs, cs)

    def moved(q, cs, to_core):
        fa, fb, fc = flips(q)
        fx = fa * (1 - cs) + fb * cs
        fy = fb * (1 - cs) + fc * cs
        fz = fc * (1 - cs) + fa * cs
        pz, py, px = ez + fz * (1 - 2 * ez), ey + fy * (1 - 2 * ey), xc + fx * (1 - 2 * xc)
        return pz, py, 2 * px + to_core

    def tok_num(p):
        return (p[0] * 2 + p[1]) * 4 + p[2]

    def exp_num(p):
        return (p[2] * 2 + p[1]) * 2 + p[0]

    barrier = pltpu.get_barrier_semaphore()

    @pl.loop(1, N_DEV)
    def _(d):
        pl.semaphore_signal(barrier, inc=1, device_id=place(d // 2, d % 2), device_id_type=MESH)

    pl.semaphore_wait(barrier, N_DEV - 1)

    def x_copy(src, slot, n, dev):
        return pltpu.make_async_remote_copy(
            src_ref=src, dst_ref=x_all.at[slot], send_sem=xs_sem.at[n], recv_sem=xr_sem.at[slot],
            device_id=dev, device_id_type=MESH)

    sib = place(0, 1)
    nbr = {1: place(1, 0), 2: place(2, 0), 3: place(3, 0)}
    for n, q in enumerate((1, 2, 3)):
        x_copy(x_ref, q, n, nbr[q]).start()
    x_copy(x_ref, 8, 3, sib).start()

    def forward(q, via, to, n):
        x_copy(x_all.at[q], to, n, nbr[via]).start()

    def push(q):
        x_copy(x_all.at[q], 8 + q, 3 + q, sib).start()

    def arrived(slot):
        x_copy(x_ref, slot, 0, sib).wait_recv()

    def meta_copy(d):
        dev = place(d // 2, d % 2)
        return pltpu.make_async_remote_copy(
            src_ref=codes_ref.at[exp_num(dev)], dst_ref=meta.at[my_tok], send_sem=ms_sem.at[d],
            recv_sem=mr_sem.at[my_tok], device_id=dev, device_id_type=MESH)

    own_meta = pltpu.make_async_copy(codes_ref.at[my_exp], meta.at[my_tok], mr_sem.at[my_tok])
    own_meta.start()

    @pl.loop(1, N_DEV)
    def _(d):
        meta_copy(d).start()

    def meta_wait(num):
        pltpu.make_async_copy(codes_ref.at[0], meta.at[num], mr_sem.at[num]).wait()

    def w_copies(e, s):
        return [pltpu.make_async_copy(w.at[e], b.at[s], w_sem.at[s, k])
                for k, (w, b) in enumerate(((w1_ref, wb1), (w3_ref, wb3), (w2_ref, wb2)))]

    for c in w_copies(0, 0):
        c.start()

    def gather(ci):
        n, q0 = 2 * UNITS[ci], FIRST[ci]

        def load(d):
            slot = q0 + d // 2 + 8 * (d % 2)
            return pltpu.make_async_copy(x_all.at[slot], xb.at[d % 2], xl_sem.at[d % 2])

        def fetch(d):
            arrived(q0 + d // 2 + 8 * (d % 2))
            load(d).start()

        if ci == 0:
            pltpu.make_async_copy(x_ref, xb.at[0], xl_sem.at[0]).start()
        else:
            load(0).start()

        @pl.loop(0, n)
        def _(d):
            @pl.when(d + 1 < n)
            def _():
                if ci == 0:
                    fetch(d + 1)
                else:
                    @pl.when((d + 1) % 2 == 1)
                    def _():
                        arrived(q0 + (d + 1) // 2 + 8)
                    load(d + 1).start()
            dev = place(q0 + d // 2, d % 2)
            num = tok_num(dev)
            meta_wait(num)
            code = meta[num]
            want = lax.broadcasted_iota(jnp.int32, (CAP, TOK), 0).astype(F32)
            sel = jnp.concatenate(
                [jnp.where(code[e:e + 1, :] == want, 1.0, 0.0).astype(BF16) for e in range(N_LOC)], axis=0)
            load(d).wait()
            at = pl.multiple_of(d * CAP, CAP)

            @pl.loop(0, HID // 512)
            def _(t):
                cols = pl.ds(pl.multiple_of(t * 512, 512), 512)
                got = jnp.dot(sel, xb[d % 2, :, cols], preferred_element_type=F32).astype(BF16)
                for e in range(N_LOC):
                    rows[e, pl.ds(at, CAP), cols] = got[e * CAP:(e + 1) * CAP]

    def ffn(ci, e):
        m = UNITS[ci] * 2 * CAP
        s = e % 2
        for c in w_copies(e, s):
            c.wait()
        def prefetch():
            for c in w_copies((e + 1) % N_LOC, 1 - s):
                c.start()
        if ci < 3:
            prefetch()
        else:
            pl.when(e + 1 < N_LOC)(prefetch)

        @pl.loop(0, FFN // 128)
        def _(t):
            cols = pl.ds(pl.multiple_of(t * 128, 128), 128)
            w = jnp.concatenate([wb1[s, :, cols], wb3[s, :, cols]], axis=1)
            h = jnp.dot(rows[e, :m, :], w, preferred_element_type=F32)
            act[:m, cols] = (jax.nn.silu(h[:, :128]) * h[:, 128:]).astype(BF16)

        @pl.loop(0, HID // 512)
        def _(t):
            cols = pl.ds(pl.multiple_of(t * 512, 512), 512)
            rows[e, :m, cols] = jnp.dot(act[:m, :], wb2[s, :, cols], preferred_element_type=F32).astype(BF16)

    def ret_copy(d):
        dev = place(d // 2, d % 2)
        return pltpu.make_async_remote_copy(
            src_ref=h_send.at[d], dst_ref=h_recv.at[my_exp], send_sem=rs_sem.at[d],
            recv_sem=rr_sem.at[my_exp], device_id=dev, device_id_type=MESH)

    def via_copy(k):
        i, c2 = k // 2, k % 2
        return pltpu.make_async_remote_copy(
            src_ref=h_send.at[2 * FIRST[2] + k], dst_ref=h_pass.at[k], send_sem=rs_sem.at[2 * FIRST[2] + k],
            recv_sem=pr_sem.at[k], device_id=place((i + 1) % 3 + 1, c2), device_id_type=MESH)

    def pass_on(k):
        i, c2 = k // 2, k % 2
        num = exp_num(moved((i + 1) % 3 + 1, core, core + c2 * (1 - 2 * core)))
        return pltpu.make_async_remote_copy(
            src_ref=h_pass.at[k], dst_ref=h_recv.at[num], send_sem=ps_sem.at[k],
            recv_sem=rr_sem.at[num], device_id=place((i + 2) % 3 + 1, 0), device_id_type=MESH)

    def stage(d):
        return pltpu.make_async_copy(sb.at[d % 2], h_send.at[d], sl_sem.at[d % 2])

    def send_back(ci):
        d0, n = 2 * FIRST[ci], 2 * UNITS[ci]

        @pl.loop(0, n)
        def _(k):
            d = d0 + k
            num = tok_num(place(d // 2, d % 2))
            pos = meta[num, 4:5, :SLOTS]
            want = lax.broadcasted_iota(jnp.int32, (RET, SLOTS), 0).astype(F32)
            sel = jnp.where(pos == want, 1.0, 0.0).astype(BF16)
            at = pl.multiple_of(k * CAP, CAP)

            @pl.loop(0, HID // 512)
            def _(t):
                cols = pl.ds(pl.multiple_of(t * 512, 512), 512)
                o = jnp.concatenate([rows[e, pl.ds(at, CAP), cols] for e in range(N_LOC)], axis=0)
                sb[d % 2, :, cols] = jnp.dot(sel, o, preferred_element_type=F32).astype(BF16)

            stage(d).start()

            @pl.when(k > 0)
            def _():
                stage(d - 1).wait()
                if ci == 1:
                    ret_copy(d - 1).start()
                elif ci == 2:
                    via_copy(k - 1).start()

        last = d0 + n - 1
        stage(last).wait()
        if ci == 2:
            via_copy(n - 1).start()
        elif ci < 2:
            ret_copy(last).start()

    def experts(ci, between=None):
        @pl.loop(0, N_LOC)
        def _(e):
            ffn(ci, e)
            if between is not None:
                pl.when(e == 2)(between)

    gather(0)
    experts(0)
    send_back(0)
    for q in (1, 2, 3):
        arrived(q)
        if q == 1:
            forward(1, 3, 5, 11)
        elif q == 2:
            forward(2, 1, 6, 12)
        else:
            forward(3, 2, 4, 13)
    for q in (1, 2, 3):
        push(q)
    gather(1)

    def relay():
        arrived(4)
        forward(4, 1, 7, 14)
        push(4)
        for q in (5, 6):
            arrived(q)
            push(q)

    experts(1, relay)
    send_back(1)
    gather(2)

    def relay_last():
        arrived(7)
        push(7)

    experts(2, relay_last)
    send_back(2)
    gather(3)
    experts(3)
    send_back(3)

    acc[...] = x_to_f32(x_ref, xb, xl_sem, acc)

    def take(d):
        num = exp_num(place(d // 2, d % 2))
        return pltpu.make_async_copy(h_recv.at[num], sb.at[d % 2], rl_sem.at[d % 2])

    def came(d):
        num = exp_num(place(d // 2, d % 2))
        pltpu.make_async_remote_copy(
            src_ref=h_send.at[d], dst_ref=h_recv.at[num], send_sem=rs_sem.at[d],
            recv_sem=rr_sem.at[num], device_id=sib, device_id_type=MESH).wait_recv()

    pltpu.make_async_copy(h_send.at[0], sb.at[0], rl_sem.at[0]).start()

    def hand_on(first):
        @pl.loop(0, 3)
        def _(i):
            via_copy(2 * i + first).wait_recv()
            pass_on(2 * i + first).start()

    def far():
        hand_on(1)
        for d in (14, 15):
            ret_copy(d).start()

    @pl.loop(0, N_DEV)
    def _(d):
        pl.when(d == 3)(lambda: hand_on(0))
        pl.when(d == 6)(far)

        @pl.when(d + 1 < N_DEV)
        def _():
            came(d + 1)
            take(d + 1).start()
        num = exp_num(place(d // 2, d % 2))
        tab = pltpu.roll(comb_ref[...], (2 * N_EXP - num * N_LOC) % (2 * N_EXP), 1)
        want = lax.broadcasted_iota(jnp.int32, (TOK, RET), 1).astype(F32)
        g = jnp.zeros((TOK, RET), F32)
        for e in range(N_LOC):
            g = jnp.where(tab[:, e:e + 1] == want, tab[:, N_EXP + e:N_EXP + e + 1], g)
        hi = g.astype(BF16)
        rest = g - hi.astype(F32)
        mid = rest.astype(BF16)
        lo = (rest - mid.astype(F32)).astype(BF16)
        lhs = jnp.concatenate([hi, mid, lo], axis=0)
        take(d).wait()

        @pl.loop(0, HID // 256)
        def _(t):
            cols = pl.ds(pl.multiple_of(t * 256, 256), 256)
            r = jnp.dot(lhs, sb[d % 2, :, cols], preferred_element_type=F32)
            acc[:, cols] += r[:TOK] + (r[TOK:2 * TOK] + r[2 * TOK:])

    y_ref[...] = acc[...].astype(BF16)
    flag_ref[...] = jnp.max(meta[:, 5:6, :128], axis=0) + jnp.zeros((8, 128), F32)

    for n in range(15):
        x_copy(x_ref, 0, n, sib).wait_send()

    @pl.loop(1, N_DEV)
    def _(d):
        meta_copy(d).wait_send()
        ret_copy(d).wait_send()

    @pl.loop(0, 6)
    def _(k):
        pass_on(k).wait_send()


def x_to_f32(x_ref, xb, xl_sem, acc):
    c = pltpu.make_async_copy(x_ref, xb.at[0], xl_sem.at[0])
    c.start()
    c.wait()
    return xb[0].astype(F32)


def moe(x, codes, comb, w1, w3, w2):
    hbm = pl.BlockSpec(memory_space=pl.ANY)
    vmem = pl.BlockSpec(memory_space=pltpu.VMEM)
    dma = pltpu.SemaphoreType.DMA
    out = pl.pallas_call(
        moe_kernel,
        out_shape=(
            jax.ShapeDtypeStruct((TOK, HID), BF16),
            jax.ShapeDtypeStruct((8, 128), F32),
            jax.ShapeDtypeStruct((N_DEV, TOK, HID), BF16),
            jax.ShapeDtypeStruct((N_DEV, RET, HID), BF16),
            jax.ShapeDtypeStruct((N_DEV, RET, HID), BF16),
            jax.ShapeDtypeStruct((6, RET, HID), BF16),
        ),
        in_specs=[hbm, hbm, vmem, hbm, hbm, hbm],
        out_specs=(vmem, vmem, hbm, hbm, hbm, hbm),
        scratch_shapes=[
            pltpu.VMEM((2, HID, FFN), BF16),
            pltpu.VMEM((2, HID, FFN), BF16),
            pltpu.VMEM((2, FFN, HID), BF16),
            pltpu.VMEM((N_LOC, 6 * CAP, HID), BF16),
            pltpu.VMEM((6 * CAP, FFN), BF16),
            pltpu.VMEM((2, TOK, HID), BF16),
            pltpu.VMEM((2, RET, HID), BF16),
            pltpu.VMEM((N_DEV, 8, TOK), F32),
            pltpu.VMEM((TOK, HID), F32),
            dma((2, 3)), dma((2,)), dma((15,)), dma((16,)), dma((16,)), dma((16,)),
            dma((2,)), dma((16,)), dma((16,)), dma((2,)), dma((6,)), dma((6,)),
        ],
        compiler_params=pltpu.CompilerParams(
            collective_id=0, has_side_effects=True, vmem_limit_bytes=67_043_328),
        name='moe',
    )(x, codes, comb, w1, w3, w2)
    return out[0], out[1]


def plain(x_loc, ids, gates, w_g, w_u, w_d):
    hit, picked, rank, gate = routing(ids, gates)
    code = jnp.where(picked, rank, -1.0)
    match = code.T.reshape(N_DEV, N_LOC, 1, TOK) == jnp.arange(CAP, dtype=F32)[None, None, :, None]
    send = jnp.einsum('slct,th->slch', match.astype(BF16), x_loc, preferred_element_type=F32).astype(BF16)
    recv = lax.all_to_all(send, EXPERT_AXES, 0, 0)

    def expert(args):
        rows, one, three, two = args
        h_gate = jnp.dot(rows, one, preferred_element_type=F32)
        h_up = jnp.dot(rows, three, preferred_element_type=F32)
        act = (jax.nn.silu(h_gate) * h_up).astype(BF16)
        return jnp.dot(act, two, preferred_element_type=F32).astype(BF16)

    out = lax.map(expert, (recv.transpose(1, 0, 2, 3).reshape(N_LOC, N_DEV * CAP, HID), w_g, w_u, w_d))
    back = lax.all_to_all(out.reshape(N_LOC, N_DEV, CAP, HID).transpose(1, 0, 2, 3), EXPERT_AXES, 0, 0)

    def add(acc, args):
        rows, code_e, gate_e = args
        share = jnp.where(code_e[:, None] == jnp.arange(CAP, dtype=F32)[None, :], gate_e[:, None], 0.0)
        return acc + jnp.dot(share, rows.astype(F32), precision=lax.Precision.HIGHEST), None

    total = lax.scan(add, x_loc.astype(F32), (back.reshape(N_EXP, CAP, HID), code.T, gate.T))[0]
    return total.astype(BF16)


def solution(mesh):
    def local_layer(x, ids, gates, w1, w3, w2):
        codes, comb = tables(ids, gates)
        y, flag = moe(x, codes, comb, w1, w3, w2)
        return lax.cond(flag[0, 0] > 0.0, lambda: plain(x, ids, gates, w1, w3, w2), lambda: y)

    tok = P(TOKEN_AXES, None)
    w = P(EXPERT_AXES, None, None)
    return jax.shard_map(local_layer, mesh=mesh, in_specs=(tok, tok, tok, w, w, w), out_specs=tok, check_vma=False)
```

```python
import functools

import jax
import jax.numpy as jnp
from jax import lax
from jax.experimental import pallas as pl
from jax.experimental.pallas import tpu as pltpu
from jax.sharding import PartitionSpec as P

TOKEN_AXES = ('ez', 'ey', 'ex')
EXPERT_AXES = ('ex', 'ey', 'ez')
MESH = pl.DeviceIdType.MESH
BF16, F32 = jnp.bfloat16, jnp.float32

N_DEV = 16
N_LOC = 4
N_EXP = N_DEV * N_LOC
TOK = 512
HID = 2048
FFN = 1408
CAP = 96
RET = 240
RET_PAD = 256
SLOTS = N_LOC * CAP
UNITS = (1, 3, 3, 1)
FIRST = (0, 1, 4, 7)


def routing(ids, gates):
    hit = ids[:, :, None] == jnp.arange(N_EXP)[None, None, :]
    picked = jnp.any(hit, axis=1)
    gate = jnp.sum(jnp.where(hit, gates[:, :, None], 0.0), axis=1)
    below = (jnp.arange(TOK)[:, None] > jnp.arange(TOK)[None, :]).astype(BF16)
    rank = jnp.dot(below, picked.astype(BF16), preferred_element_type=F32)
    return hit, picked, rank, gate


def tables(ids, gates):
    hit, picked, rank, gate = routing(ids, gates)
    cnt = jnp.sum(picked.astype(F32), axis=0).reshape(N_DEV, N_LOC)
    tri = (jnp.arange(N_LOC)[:, None] > jnp.arange(N_LOC)[None, :]).astype(F32)
    off = jnp.sum(cnt[:, None, :] * tri[None], axis=-1)
    over = jnp.max(jnp.sum(cnt, axis=1)) > RET
    code = jnp.where(picked, rank, -1.0).T.reshape(N_DEV, N_LOC, TOK)
    slot = jnp.arange(CAP, dtype=F32)
    pos = jnp.where(slot < cnt[:, :, None], off[:, :, None] + slot, -1.0).reshape(N_DEV, 1, SLOTS)
    pos = jnp.pad(pos, ((0, 0), (0, 0), (0, TOK - SLOTS)), constant_values=-1.0)
    flag = jnp.broadcast_to(over.astype(F32), (N_DEV, 3, TOK))
    codes = jnp.concatenate([code, pos, flag], axis=1)
    place = jnp.where(picked, off.reshape(-1)[None] + rank, -1.0)
    comb = jnp.concatenate([place, gate], axis=1)
    return codes, comb


def flips(q):
    ct, i = (q + 2) // 3, (q + 2) % 3
    w1, w2, w3 = (ct % 2) * (1 - ct // 2), (1 - ct % 2) * (ct // 2), (ct % 2) * (ct // 2)
    base = ((3 - i) // 3, i % 2, i // 2)
    return tuple(w1 * f + w2 * (1 - f) + w3 for f in base)


def moe_kernel(x_ref, codes_ref, comb_ref, w1_ref, w3_ref, w2_ref,
               y_ref, flag_ref, x_all, h_send, h_recv, h_pass,
               wb1, wb3, wb2, rows, act, xb, sb, meta, acc,
               w_sem, xl_sem, xs_sem, xr_sem, ms_sem, mr_sem, sl_sem, rs_sem, rr_sem, rl_sem, ps_sem, pr_sem):
    ez, ey, ex = (lax.axis_index(a) for a in TOKEN_AXES)
    core, xc = ex % 2, ex // 2
    my_tok = (ez * 2 + ey) * 4 + ex
    my_exp = (ex * 2 + ey) * 2 + ez

    def place(q, other):
        cs = core + other * (1 - 2 * core)
        return moved(q, cs, cs)

    def moved(q, cs, to_core):
        fa, fb, fc = flips(q)
        fx = fa * (1 - cs) + fb * cs
        fy = fb * (1 - cs) + fc * cs
        fz = fc * (1 - cs) + fa * cs
        pz, py, px = ez + fz * (1 - 2 * ez), ey + fy * (1 - 2 * ey), xc + fx * (1 - 2 * xc)
        return pz, py, 2 * px + to_core

    def tok_num(p):
        return (p[0] * 2 + p[1]) * 4 + p[2]

    def exp_num(p):
        return (p[2] * 2 + p[1]) * 2 + p[0]

    barrier = pltpu.get_barrier_semaphore()

    @pl.loop(1, N_DEV)
    def _(d):
        pl.semaphore_signal(barrier, inc=1, device_id=place(d // 2, d % 2), device_id_type=MESH)

    pl.semaphore_wait(barrier, N_DEV - 1)

    def x_copy(src, slot, n, dev):
        return pltpu.make_async_remote_copy(
            src_ref=src, dst_ref=x_all.at[slot], send_sem=xs_sem.at[n], recv_sem=xr_sem.at[slot],
            device_id=dev, device_id_type=MESH)

    sib = place(0, 1)
    nbr = {1: place(1, 0), 2: place(2, 0), 3: place(3, 0)}
    for n, q in enumerate((1, 2, 3)):
        x_copy(x_ref, q, n, nbr[q]).start()
    x_copy(x_ref, 8, 3, sib).start()

    def forward(q, via, to, n):
        x_copy(x_all.at[q], to, n, nbr[via]).start()

    def push(q):
        x_copy(x_all.at[q], 8 + q, 3 + q, sib).start()

    def arrived(slot):
        x_copy(x_ref, slot, 0, sib).wait_recv()

    def meta_copy(d):
        dev = place(d // 2, d % 2)
        return pltpu.make_async_remote_copy(
            src_ref=codes_ref.at[exp_num(dev)], dst_ref=meta.at[my_tok], send_sem=ms_sem.at[d],
            recv_sem=mr_sem.at[my_tok], device_id=dev, device_id_type=MESH)

    own_meta = pltpu.make_async_copy(codes_ref.at[my_exp], meta.at[my_tok], mr_sem.at[my_tok])
    own_meta.start()

    @pl.loop(1, N_DEV)
    def _(d):
        meta_copy(d).start()

    def meta_wait(num):
        pltpu.make_async_copy(codes_ref.at[0], meta.at[num], mr_sem.at[num]).wait()

    def w_copies(e, s):
        return [pltpu.make_async_copy(w.at[e], b.at[s], w_sem.at[s, k])
                for k, (w, b) in enumerate(((w1_ref, wb1), (w3_ref, wb3), (w2_ref, wb2)))]

    for c in w_copies(0, 0):
        c.start()
    sb[:, RET:, :] = jnp.zeros((2, RET_PAD - RET, HID), BF16)

    def gather(ci):
        nu, q0 = UNITS[ci], FIRST[ci]
        n = 2 * nu

        def load(g):
            src = x_all.at[q0 + g % nu + 8 * (g // nu)]
            return pltpu.make_async_copy(src, xb.at[g % 3], xl_sem.at[g % 3])

        def fetch(g):
            @pl.when(g >= nu)
            def _():
                arrived(q0 + g % nu + 8)
            load(g).start()

        if ci == 0:
            pltpu.make_async_copy(x_ref, xb.at[0], xl_sem.at[0]).start()
        else:
            fetch(0)
        fetch(1)

        @pl.loop(0, n)
        def _(g):
            @pl.when(g + 2 < n)
            def _():
                fetch(g + 2)
            d = 2 * (g % nu) + g // nu
            dev = place(q0 + d // 2, d % 2)
            num = tok_num(dev)
            meta_wait(num)
            code = meta[num]
            want = lax.broadcasted_iota(jnp.int32, (CAP, TOK), 0).astype(F32)
            sel = jnp.concatenate(
                [jnp.where(code[e:e + 1, :] == want, 1.0, 0.0).astype(BF16) for e in range(N_LOC)], axis=0)
            load(g).wait()
            at = pl.multiple_of(d * CAP, CAP)

            @pl.loop(0, HID // 1024)
            def _(t):
                cols = pl.ds(pl.multiple_of(t * 1024, 1024), 1024)
                got = jnp.dot(sel, xb[g % 3, :, cols], preferred_element_type=F32).astype(BF16)
                for e in range(N_LOC):
                    rows[e, pl.ds(at, CAP), cols] = got[e * CAP:(e + 1) * CAP]

    def ffn(ci, e):
        m = UNITS[ci] * 2 * CAP
        s = e % 2
        for c in w_copies(e, s):
            c.wait()
        def prefetch():
            for c in w_copies((e + 1) % N_LOC, 1 - s):
                c.start()
        if ci < 3:
            prefetch()
        else:
            pl.when(e + 1 < N_LOC)(prefetch)

        def up(at, wide):
            cols = pl.ds(at, wide)
            w = jnp.concatenate([wb1[s, :, cols], wb3[s, :, cols]], axis=1)
            h = jnp.dot(rows[e, :m, :], w, preferred_element_type=F32)
            act[:m, cols] = (jax.nn.silu(h[:, :wide]) * h[:, wide:]).astype(BF16)

        @pl.loop(0, FFN // 256)
        def _(t):
            up(pl.multiple_of(t * 256, 256), 256)

        up(FFN // 256 * 256, FFN % 256)

        @pl.loop(0, HID // 1024)
        def _(t):
            cols = pl.ds(pl.multiple_of(t * 1024, 1024), 1024)
            rows[e, :m, cols] = jnp.dot(act[:m, :], wb2[s, :, cols], preferred_element_type=F32).astype(BF16)

    def ret_copy(d):
        dev = place(d // 2, d % 2)
        return pltpu.make_async_remote_copy(
            src_ref=h_send.at[d], dst_ref=h_recv.at[my_exp], send_sem=rs_sem.at[d],
            recv_sem=rr_sem.at[my_exp], device_id=dev, device_id_type=MESH)

    def via_copy(k):
        i, c2 = k // 2, k % 2
        return pltpu.make_async_remote_copy(
            src_ref=h_send.at[2 * FIRST[2] + k], dst_ref=h_pass.at[k], send_sem=rs_sem.at[2 * FIRST[2] + k],
            recv_sem=pr_sem.at[k], device_id=place((i + 1) % 3 + 1, c2), device_id_type=MESH)

    def pass_on(k):
        i, c2 = k // 2, k % 2
        num = exp_num(moved((i + 1) % 3 + 1, core, core + c2 * (1 - 2 * core)))
        return pltpu.make_async_remote_copy(
            src_ref=h_pass.at[k], dst_ref=h_recv.at[num], send_sem=ps_sem.at[k],
            recv_sem=rr_sem.at[num], device_id=place((i + 2) % 3 + 1, 0), device_id_type=MESH)

    def stage(d):
        return pltpu.make_async_copy(sb.at[d % 2, pl.ds(0, RET)], h_send.at[d], sl_sem.at[d % 2])

    def send_back(ci):
        d0, n = 2 * FIRST[ci], 2 * UNITS[ci]

        @pl.loop(0, n)
        def _(k):
            d = d0 + k
            num = tok_num(place(d // 2, d % 2))
            pos = meta[num, 4:5, :SLOTS]
            want = lax.broadcasted_iota(jnp.int32, (RET, SLOTS), 0).astype(F32)
            sel = jnp.where(pos == want, 1.0, 0.0).astype(BF16)
            at = pl.multiple_of(k * CAP, CAP)

            @pl.loop(0, HID // 1024)
            def _(t):
                cols = pl.ds(pl.multiple_of(t * 1024, 1024), 1024)
                o = jnp.concatenate([rows[e, pl.ds(at, CAP), cols] for e in range(N_LOC)], axis=0)
                sb[d % 2, :RET, cols] = jnp.dot(sel, o, preferred_element_type=F32).astype(BF16)

            stage(d).start()

            @pl.when(k > 0)
            def _():
                stage(d - 1).wait()
                if ci == 1:
                    ret_copy(d - 1).start()
                elif ci == 2:
                    via_copy(k - 1).start()

        last = d0 + n - 1
        stage(last).wait()
        if ci == 2:
            via_copy(n - 1).start()
        elif ci < 2:
            ret_copy(last).start()

    def hand_on(first):
        @pl.loop(0, 3)
        def _(i):
            with jax.named_scope('hand'):
                via_copy(2 * i + first).wait_recv()
            pass_on(2 * i + first).start()

    def experts(ci, between=None):
        @pl.loop(0, N_LOC)
        def _(e):
            ffn(ci, e)
            if between is not None:
                pl.when(e == 2)(between)

    ns = jax.named_scope
    with ns('gather0'):
        gather(0)
    with ns('ffn0'):
        experts(0)
    with ns('send0'):
        send_back(0)
    with ns('wait_x1'):
        for q in (1, 2, 3):
            arrived(q)
            if q == 1:
                forward(1, 3, 5, 11)
            elif q == 2:
                forward(2, 1, 6, 12)
            else:
                forward(3, 2, 4, 13)
        for q in (1, 2, 3):
            push(q)
    with ns('gather1'):
        gather(1)

    def relay():
        with ns('wait_x2'):
            arrived(4)
            forward(4, 1, 7, 14)
            push(4)
            for q in (5, 6):
                arrived(q)
                push(q)

    with ns('ffn1'):
        experts(1, relay)
    with ns('send1'):
        send_back(1)
    with ns('gather2'):
        gather(2)

    def relay_last():
        with ns('wait_x3'):
            arrived(7)
            push(7)

    with ns('ffn2'):
        experts(2, relay_last)
    with ns('send2'):
        send_back(2)
    with ns('gather3'):
        gather(3)
    with ns('ffn3'):
        experts(3, lambda: hand_on(0))
    with ns('send3'):
        send_back(3)

    acc[...] = x_to_f32(x_ref, xb, xl_sem, acc)

    def take(d):
        num = exp_num(place(d // 2, d % 2))
        return pltpu.make_async_copy(h_recv.at[num], sb.at[d % 2, pl.ds(0, RET)], rl_sem.at[d % 2])

    def came(d):
        num = exp_num(place(d // 2, d % 2))
        pltpu.make_async_remote_copy(
            src_ref=h_send.at[d], dst_ref=h_recv.at[num], send_sem=rs_sem.at[d],
            recv_sem=rr_sem.at[num], device_id=sib, device_id_type=MESH).wait_recv()

    pltpu.make_async_copy(h_send.at[0], sb.at[0, pl.ds(0, RET)], rl_sem.at[0]).start()

    def far():
        hand_on(1)
        for d in (14, 15):
            ret_copy(d).start()

    @pl.loop(0, N_DEV)
    def _(d):
        pl.when(d == 3)(far)

        @pl.when(d + 1 < N_DEV)
        def _():
            with jax.named_scope('came'):
                came(d + 1)
            take(d + 1).start()
        num = exp_num(place(d // 2, d % 2))
        tab = pltpu.roll(comb_ref[...], (2 * N_EXP - num * N_LOC) % (2 * N_EXP), 1)
        want = lax.broadcasted_iota(jnp.int32, (TOK, RET_PAD), 1).astype(F32)
        g = jnp.zeros((TOK, RET_PAD), F32)
        for e in range(N_LOC):
            g = jnp.where(tab[:, e:e + 1] == want, tab[:, N_EXP + e:N_EXP + e + 1], g)
        hi = g.astype(BF16)
        rest = g - hi.astype(F32)
        mid = rest.astype(BF16)
        lo = (rest - mid.astype(F32)).astype(BF16)
        lhs = jnp.concatenate([hi, mid, lo], axis=1)
        take(d).wait()

        @pl.loop(0, HID // 512)
        def _(t):
            cols = pl.ds(pl.multiple_of(t * 512, 512), 512)
            back = sb[d % 2, :, cols]
            acc[:, cols] += jnp.dot(lhs, jnp.concatenate([back] * 3, axis=0), preferred_element_type=F32)

    y_ref[...] = acc[...].astype(BF16)
    flag_ref[...] = jnp.max(meta[:, 5:6, :128], axis=0) + jnp.zeros((8, 128), F32)

    for n in range(15):
        x_copy(x_ref, 0, n, sib).wait_send()

    @pl.loop(1, N_DEV)
    def _(d):
        meta_copy(d).wait_send()
        ret_copy(d).wait_send()

    @pl.loop(0, 6)
    def _(k):
        pass_on(k).wait_send()


def x_to_f32(x_ref, xb, xl_sem, acc):
    c = pltpu.make_async_copy(x_ref, xb.at[0], xl_sem.at[0])
    c.start()
    c.wait()
    return xb[0].astype(F32)


def moe(x, codes, comb, w1, w3, w2):
    hbm = pl.BlockSpec(memory_space=pl.ANY)
    vmem = pl.BlockSpec(memory_space=pltpu.VMEM)
    dma = pltpu.SemaphoreType.DMA
    out = pl.pallas_call(
        moe_kernel,
        out_shape=(
            jax.ShapeDtypeStruct((TOK, HID), BF16),
            jax.ShapeDtypeStruct((8, 128), F32),
            jax.ShapeDtypeStruct((N_DEV, TOK, HID), BF16),
            jax.ShapeDtypeStruct((N_DEV, RET, HID), BF16),
            jax.ShapeDtypeStruct((N_DEV, RET, HID), BF16),
            jax.ShapeDtypeStruct((6, RET, HID), BF16),
        ),
        in_specs=[hbm, hbm, vmem, hbm, hbm, hbm],
        out_specs=(vmem, vmem, hbm, hbm, hbm, hbm),
        scratch_shapes=[
            pltpu.VMEM((2, HID, FFN), BF16),
            pltpu.VMEM((2, HID, FFN), BF16),
            pltpu.VMEM((2, FFN, HID), BF16),
            pltpu.VMEM((N_LOC, 6 * CAP, HID), BF16),
            pltpu.VMEM((6 * CAP, FFN), BF16),
            pltpu.VMEM((3, TOK, HID), BF16),
            pltpu.VMEM((2, RET_PAD, HID), BF16),
            pltpu.VMEM((N_DEV, 8, TOK), F32),
            pltpu.VMEM((TOK, HID), F32),
            dma((2, 3)), dma((3,)), dma((15,)), dma((16,)), dma((16,)), dma((16,)),
            dma((2,)), dma((16,)), dma((16,)), dma((2,)), dma((6,)), dma((6,)),
        ],
        compiler_params=pltpu.CompilerParams(
            collective_id=0, has_side_effects=True, vmem_limit_bytes=67_043_328),
        name='moe',
    )(x, codes, comb, w1, w3, w2)
    return out[0], out[1]


def plain(x_loc, ids, gates, w_g, w_u, w_d):
    hit, picked, rank, gate = routing(ids, gates)
    code = jnp.where(picked, rank, -1.0)
    match = code.T.reshape(N_DEV, N_LOC, 1, TOK) == jnp.arange(CAP, dtype=F32)[None, None, :, None]
    send = jnp.einsum('slct,th->slch', match.astype(BF16), x_loc, preferred_element_type=F32).astype(BF16)
    recv = lax.all_to_all(send, EXPERT_AXES, 0, 0)

    def expert(args):
        rows, one, three, two = args
        h_gate = jnp.dot(rows, one, preferred_element_type=F32)
        h_up = jnp.dot(rows, three, preferred_element_type=F32)
        act = (jax.nn.silu(h_gate) * h_up).astype(BF16)
        return jnp.dot(act, two, preferred_element_type=F32).astype(BF16)

    out = lax.map(expert, (recv.transpose(1, 0, 2, 3).reshape(N_LOC, N_DEV * CAP, HID), w_g, w_u, w_d))
    back = lax.all_to_all(out.reshape(N_LOC, N_DEV, CAP, HID).transpose(1, 0, 2, 3), EXPERT_AXES, 0, 0)

    def add(acc, args):
        rows, code_e, gate_e = args
        share = jnp.where(code_e[:, None] == jnp.arange(CAP, dtype=F32)[None, :], gate_e[:, None], 0.0)
        return acc + jnp.dot(share, rows.astype(F32), precision=lax.Precision.HIGHEST), None

    total = lax.scan(add, x_loc.astype(F32), (back.reshape(N_EXP, CAP, HID), code.T, gate.T))[0]
    return total.astype(BF16)


def solution(mesh):
    def local_layer(x, ids, gates, w1, w3, w2):
        codes, comb = tables(ids, gates)
        y, flag = moe(x, codes, comb, w1, w3, w2)
        return lax.cond(flag[0, 0] > 0.0, lambda: plain(x, ids, gates, w1, w3, w2), lambda: y)

    tok = P(TOKEN_AXES, None)
    w = P(EXPERT_AXES, None, None)
    return jax.shard_map(local_layer, mesh=mesh, in_specs=(tok, tok, tok, w, w, w), out_specs=tok, check_vma=False)
```

```python
import functools

import jax
import jax.numpy as jnp
from jax import lax
from jax.experimental import pallas as pl
from jax.experimental.pallas import tpu as pltpu
from jax.sharding import PartitionSpec as P

TOKEN_AXES = ('ez', 'ey', 'ex')
EXPERT_AXES = ('ex', 'ey', 'ez')
MESH = pl.DeviceIdType.MESH
BF16, F32 = jnp.bfloat16, jnp.float32

N_DEV = 16
N_LOC = 4
N_EXP = N_DEV * N_LOC
TOK = 512
HID = 2048
FFN = 1408
CAP = 96
RET = 240
RET_PAD = 256
SLOTS = N_LOC * CAP
UNITS = (1, 3, 3, 1)
FIRST = (0, 1, 4, 7)


def routing(ids, gates):
    hit = ids[:, :, None] == jnp.arange(N_EXP)[None, None, :]
    picked = jnp.any(hit, axis=1)
    gate = jnp.sum(jnp.where(hit, gates[:, :, None], 0.0), axis=1)
    below = (jnp.arange(TOK)[:, None] > jnp.arange(TOK)[None, :]).astype(BF16)
    rank = jnp.dot(below, picked.astype(BF16), preferred_element_type=F32)
    return hit, picked, rank, gate


def iota(shape, axis):
    return lax.broadcasted_iota(jnp.int32, shape, axis)


def one(mask):
    return jnp.where(mask, 1.0, 0.0)


def send_tables(ids_t):
    picked = jnp.zeros((N_EXP, TOK), F32)
    for k in range(ids_t.shape[0]):
        picked = picked + one(ids_t[k:k + 1, :] == iota((N_EXP, TOK), 0))
    before = one(iota((TOK, TOK), 0) < iota((TOK, TOK), 1)).astype(BF16)
    rank = jnp.dot(picked.astype(BF16), before, preferred_element_type=F32)
    code = jnp.where(picked > 0.0, rank, -1.0)
    r, c = iota((N_EXP, N_EXP), 0), iota((N_EXP, N_EXP), 1)
    mine = one(r // N_LOC == c // N_LOC)
    lower = one((r // N_LOC == c // N_LOC) & (c < r))
    hot = picked.astype(BF16)
    cnt = jnp.sum(picked, axis=1, keepdims=True)
    off = jnp.sum(jnp.dot(lower.astype(BF16), hot, preferred_element_type=F32), axis=1, keepdims=True)
    full = jnp.sum(jnp.dot(mine.astype(BF16), hot, preferred_element_type=F32), axis=1, keepdims=True)
    over = jnp.max(one(full > RET), axis=0, keepdims=True)
    slot = iota((N_EXP, TOK), 1) - (iota((N_EXP, TOK), 0) % N_LOC) * CAP
    at = slot.astype(F32)
    used = (slot >= 0) & (slot < CAP) & (at < cnt)
    pos = jnp.where(used, off + at + 1.0, 0.0)
    return code, jnp.where(iota((N_EXP, TOK), 1) < SLOTS, pos, over)


def back_table(ids, gates):
    picked = jnp.zeros((TOK, N_EXP), F32)
    gate = jnp.zeros((TOK, N_EXP), F32)
    for k in range(ids.shape[1]):
        hit = ids[:, k:k + 1] == iota((TOK, N_EXP), 1)
        picked = picked + one(hit)
        gate = jnp.where(hit, gates[:, k:k + 1], gate)
    hot = picked.astype(BF16)
    after = one(iota((TOK, TOK), 0) > iota((TOK, TOK), 1)).astype(BF16)
    rank = jnp.dot(after, hot, preferred_element_type=F32)
    r, c = iota((N_EXP, N_EXP), 0), iota((N_EXP, N_EXP), 1)
    upper = one((r // N_LOC == c // N_LOC) & (r < c)).astype(BF16)
    off = jnp.sum(jnp.dot(hot, upper, preferred_element_type=F32), axis=0, keepdims=True)
    return jnp.concatenate([jnp.where(picked > 0.0, off + rank, -1.0), gate], axis=1)


def flips(q):
    ct, i = (q + 2) // 3, (q + 2) % 3
    w1, w2, w3 = (ct % 2) * (1 - ct // 2), (1 - ct % 2) * (ct // 2), (ct % 2) * (ct // 2)
    base = ((3 - i) // 3, i % 2, i // 2)
    return tuple(w1 * f + w2 * (1 - f) + w3 for f in base)


def moe_kernel(x_ref, ids_ref, idt_ref, gates_ref, w1_ref, w3_ref, w2_ref,
               y_ref, flag_ref, x_all, h_send, h_recv, h_pass,
               wb1, wb3, wb2, rows, act, xb, sb, meta, codes, comb, acc,
               w_sem, xl_sem, xs_sem, xr_sem, ms_sem, mr_sem, sl_sem, rs_sem, rr_sem, rl_sem, ps_sem, pr_sem):
    ez, ey, ex = (lax.axis_index(a) for a in TOKEN_AXES)
    core, xc = ex % 2, ex // 2
    my_tok = (ez * 2 + ey) * 4 + ex
    my_exp = (ex * 2 + ey) * 2 + ez

    def place(q, other):
        cs = core + other * (1 - 2 * core)
        return moved(q, cs, cs)

    def moved(q, cs, to_core):
        fa, fb, fc = flips(q)
        fx = fa * (1 - cs) + fb * cs
        fy = fb * (1 - cs) + fc * cs
        fz = fc * (1 - cs) + fa * cs
        pz, py, px = ez + fz * (1 - 2 * ez), ey + fy * (1 - 2 * ey), xc + fx * (1 - 2 * xc)
        return pz, py, 2 * px + to_core

    def tok_num(p):
        return (p[0] * 2 + p[1]) * 4 + p[2]

    def exp_num(p):
        return (p[2] * 2 + p[1]) * 2 + p[0]

    barrier = pltpu.get_barrier_semaphore()

    @pl.loop(1, N_DEV)
    def _(d):
        pl.semaphore_signal(barrier, inc=1, device_id=place(d // 2, d % 2), device_id_type=MESH)

    pl.semaphore_wait(barrier, N_DEV - 1)

    def x_copy(src, slot, n, dev):
        return pltpu.make_async_remote_copy(
            src_ref=src, dst_ref=x_all.at[slot], send_sem=xs_sem.at[n], recv_sem=xr_sem.at[slot],
            device_id=dev, device_id_type=MESH)

    sib = place(0, 1)
    nbr = {1: place(1, 0), 2: place(2, 0), 3: place(3, 0)}
    for n, q in enumerate((1, 2, 3)):
        x_copy(x_ref, q, n, nbr[q]).start()
    x_copy(x_ref, 8, 3, sib).start()

    def forward(q, via, to, n):
        x_copy(x_all.at[q], to, n, nbr[via]).start()

    def push(q):
        x_copy(x_all.at[q], 8 + q, 3 + q, sib).start()

    def arrived(slot):
        x_copy(x_ref, slot, 0, sib).wait_recv()

    def w_copies(e, s):
        return [pltpu.make_async_copy(w.at[e], b.at[s], w_sem.at[s, k])
                for k, (w, b) in enumerate(((w1_ref, wb1), (w3_ref, wb3), (w2_ref, wb2)))]

    for c in w_copies(0, 0):
        c.start()
    sb[:, RET:, :] = jnp.zeros((2, RET_PAD - RET, HID), BF16)

    def meta_copy(d):
        dev = place(d // 2, d % 2)
        return pltpu.make_async_remote_copy(
            src_ref=codes.at[exp_num(dev)], dst_ref=meta.at[my_tok], send_sem=ms_sem.at[d],
            recv_sem=mr_sem.at[my_tok], device_id=dev, device_id_type=MESH)

    code, pos = send_tables(idt_ref[...])
    for e in range(N_DEV):
        part = slice(e * N_LOC, (e + 1) * N_LOC)
        codes[e] = jnp.concatenate([code[part], pos[part]], axis=0)
    comb[...] = back_table(ids_ref[...], gates_ref[...])
    meta[my_tok] = codes[my_exp]

    @pl.loop(1, N_DEV)
    def _(d):
        meta_copy(d).start()

    def meta_wait(num):
        pltpu.make_async_remote_copy(
            src_ref=codes.at[0], dst_ref=meta.at[num], send_sem=ms_sem.at[0], recv_sem=mr_sem.at[num],
            device_id=sib, device_id_type=MESH).wait_recv()

    def gather(ci):
        nu, q0 = UNITS[ci], FIRST[ci]
        n = 2 * nu

        def load(g):
            src = x_all.at[q0 + g % nu + 8 * (g // nu)]
            return pltpu.make_async_copy(src, xb.at[g % 3], xl_sem.at[g % 3])

        def fetch(g):
            @pl.when(g >= nu)
            def _():
                arrived(q0 + g % nu + 8)
            load(g).start()

        if ci == 0:
            pltpu.make_async_copy(x_ref, xb.at[0], xl_sem.at[0]).start()
        else:
            fetch(0)
        fetch(1)

        @pl.loop(0, n)
        def _(g):
            @pl.when(g + 2 < n)
            def _():
                fetch(g + 2)
            d = 2 * (g % nu) + g // nu
            dev = place(q0 + d // 2, d % 2)
            num = tok_num(dev)
            if ci == 0:
                pl.when(g > 0)(lambda: meta_wait(num))
            else:
                meta_wait(num)
            code = meta[num]
            want = lax.broadcasted_iota(jnp.int32, (CAP, TOK), 0).astype(F32)
            sel = jnp.concatenate(
                [jnp.where(code[e:e + 1, :] == want, 1.0, 0.0).astype(BF16) for e in range(N_LOC)], axis=0)
            load(g).wait()
            at = pl.multiple_of(d * CAP, CAP)

            @pl.loop(0, HID // 1024)
            def _(t):
                cols = pl.ds(pl.multiple_of(t * 1024, 1024), 1024)
                got = jnp.dot(sel, xb[g % 3, :, cols], preferred_element_type=F32).astype(BF16)
                for e in range(N_LOC):
                    rows[e, pl.ds(at, CAP), cols] = got[e * CAP:(e + 1) * CAP]

    def ffn(ci, e):
        m = UNITS[ci] * 2 * CAP
        s = e % 2
        for c in w_copies(e, s):
            c.wait()
        def prefetch():
            for c in w_copies((e + 1) % N_LOC, 1 - s):
                c.start()
        if ci < 3:
            prefetch()
        else:
            pl.when(e + 1 < N_LOC)(prefetch)

        def up(at, wide):
            cols = pl.ds(at, wide)
            w = jnp.concatenate([wb1[s, :, cols], wb3[s, :, cols]], axis=1)
            h = jnp.dot(rows[e, :m, :], w, preferred_element_type=F32)
            act[:m, cols] = (jax.nn.silu(h[:, :wide]) * h[:, wide:]).astype(BF16)

        @pl.loop(0, FFN // 256)
        def _(t):
            up(pl.multiple_of(t * 256, 256), 256)

        up(FFN // 256 * 256, FFN % 256)

        @pl.loop(0, HID // 1024)
        def _(t):
            cols = pl.ds(pl.multiple_of(t * 1024, 1024), 1024)
            rows[e, :m, cols] = jnp.dot(act[:m, :], wb2[s, :, cols], preferred_element_type=F32).astype(BF16)

    def ret_copy(d):
        dev = place(d // 2, d % 2)
        return pltpu.make_async_remote_copy(
            src_ref=h_send.at[d], dst_ref=h_recv.at[my_exp], send_sem=rs_sem.at[d],
            recv_sem=rr_sem.at[my_exp], device_id=dev, device_id_type=MESH)

    def via_copy(k):
        i, c2 = k // 2, k % 2
        return pltpu.make_async_remote_copy(
            src_ref=h_send.at[2 * FIRST[2] + k], dst_ref=h_pass.at[k], send_sem=rs_sem.at[2 * FIRST[2] + k],
            recv_sem=pr_sem.at[k], device_id=place((i + 1) % 3 + 1, c2), device_id_type=MESH)

    def pass_on(k):
        i, c2 = k // 2, k % 2
        num = exp_num(moved((i + 1) % 3 + 1, core, core + c2 * (1 - 2 * core)))
        return pltpu.make_async_remote_copy(
            src_ref=h_pass.at[k], dst_ref=h_recv.at[num], send_sem=ps_sem.at[k],
            recv_sem=rr_sem.at[num], device_id=place((i + 2) % 3 + 1, 0), device_id_type=MESH)

    def stage(d):
        return pltpu.make_async_copy(sb.at[d % 2, pl.ds(0, RET)], h_send.at[d], sl_sem.at[d % 2])

    def send_back(ci):
        d0, n = 2 * FIRST[ci], 2 * UNITS[ci]

        @pl.loop(0, n)
        def _(k):
            d = d0 + k
            num = tok_num(place(d // 2, d % 2))
            pos = jnp.sum(meta[num, 4:8, :SLOTS], axis=0, keepdims=True) - 1.0
            want = lax.broadcasted_iota(jnp.int32, (RET, SLOTS), 0).astype(F32)
            sel = jnp.where(pos == want, 1.0, 0.0).astype(BF16)
            at = pl.multiple_of(k * CAP, CAP)

            @pl.loop(0, HID // 1024)
            def _(t):
                cols = pl.ds(pl.multiple_of(t * 1024, 1024), 1024)
                o = jnp.concatenate([rows[e, pl.ds(at, CAP), cols] for e in range(N_LOC)], axis=0)
                sb[d % 2, :RET, cols] = jnp.dot(sel, o, preferred_element_type=F32).astype(BF16)

            stage(d).start()

            @pl.when(k > 0)
            def _():
                stage(d - 1).wait()
                if ci == 1:
                    ret_copy(d - 1).start()
                elif ci == 2:
                    via_copy(k - 1).start()

        last = d0 + n - 1
        stage(last).wait()
        if ci == 2:
            via_copy(n - 1).start()
        elif ci < 2:
            ret_copy(last).start()

    def hand_on(first):
        @pl.loop(0, 3)
        def _(i):
            with jax.named_scope('hand'):
                via_copy(2 * i + first).wait_recv()
            pass_on(2 * i + first).start()

    def experts(ci, between=None):
        @pl.loop(0, N_LOC)
        def _(e):
            ffn(ci, e)
            if between is not None:
                pl.when(e == 2)(between)

    ns = jax.named_scope
    with ns('gather0'):
        gather(0)
    with ns('ffn0'):
        experts(0)
    with ns('send0'):
        send_back(0)
    with ns('wait_x1'):
        for q in (1, 2, 3):
            arrived(q)
            if q == 1:
                forward(1, 3, 5, 11)
            elif q == 2:
                forward(2, 1, 6, 12)
            else:
                forward(3, 2, 4, 13)
        for q in (1, 2, 3):
            push(q)
    with ns('gather1'):
        gather(1)

    def relay():
        with ns('wait_x2'):
            arrived(4)
            forward(4, 1, 7, 14)
            push(4)
            for q in (5, 6):
                arrived(q)
                push(q)

    with ns('ffn1'):
        experts(1, relay)
    with ns('send1'):
        send_back(1)
    with ns('gather2'):
        gather(2)

    def relay_last():
        with ns('wait_x3'):
            arrived(7)
            push(7)

    with ns('ffn2'):
        experts(2, relay_last)
    with ns('send2'):
        send_back(2)
    with ns('gather3'):
        gather(3)
    with ns('ffn3'):
        experts(3)
    with ns('send3'):
        send_back(3)

    acc[...] = x_to_f32(x_ref, xb, xl_sem, acc)

    def take(d):
        num = exp_num(place(d // 2, d % 2))
        return pltpu.make_async_copy(h_recv.at[num], sb.at[d % 2, pl.ds(0, RET)], rl_sem.at[d % 2])

    def came(d):
        num = exp_num(place(d // 2, d % 2))
        pltpu.make_async_remote_copy(
            src_ref=h_send.at[d], dst_ref=h_recv.at[num], send_sem=rs_sem.at[d],
            recv_sem=rr_sem.at[num], device_id=sib, device_id_type=MESH).wait_recv()

    pltpu.make_async_copy(h_send.at[0], sb.at[0, pl.ds(0, RET)], rl_sem.at[0]).start()

    def far():
        hand_on(1)
        for d in (14, 15):
            ret_copy(d).start()

    @pl.loop(0, N_DEV)
    def _(d):
        pl.when(d == 2)(lambda: hand_on(0))
        pl.when(d == 5)(far)

        @pl.when(d + 1 < N_DEV)
        def _():
            with jax.named_scope('came'):
                came(d + 1)
            take(d + 1).start()
        num = exp_num(place(d // 2, d % 2))
        tab = pltpu.roll(comb[...], (2 * N_EXP - num * N_LOC) % (2 * N_EXP), 1)
        want = lax.broadcasted_iota(jnp.int32, (TOK, RET_PAD), 1).astype(F32)
        g = jnp.zeros((TOK, RET_PAD), F32)
        for e in range(N_LOC):
            g = jnp.where(tab[:, e:e + 1] == want, tab[:, N_EXP + e:N_EXP + e + 1], g)
        hi = g.astype(BF16)
        rest = g - hi.astype(F32)
        mid = rest.astype(BF16)
        lo = (rest - mid.astype(F32)).astype(BF16)
        lhs = jnp.concatenate([hi, mid, lo], axis=1)
        take(d).wait()

        @pl.loop(0, HID // 512)
        def _(t):
            cols = pl.ds(pl.multiple_of(t * 512, 512), 512)
            back = sb[d % 2, :, cols]
            acc[:, cols] += jnp.dot(lhs, jnp.concatenate([back] * 3, axis=0), preferred_element_type=F32)

    out = [pltpu.make_async_copy(xb.at[1, pl.ds(h * 256, 256)], y_ref.at[pl.ds(h * 256, 256)], xl_sem.at[h])
           for h in range(2)]
    for h in range(2):
        xb[1, h * 256:(h + 1) * 256, :] = acc[h * 256:(h + 1) * 256, :].astype(BF16)
        out[h].start()
    flag_ref[0, 0] = jnp.max(meta[:, 4, SLOTS:])

    for c in out:
        c.wait()
    for n in range(15):
        x_copy(x_ref, 0, n, sib).wait_send()

    @pl.loop(1, N_DEV)
    def _(d):
        meta_copy(d).wait_send()
        ret_copy(d).wait_send()

    @pl.loop(0, 6)
    def _(k):
        pass_on(k).wait_send()


def x_to_f32(x_ref, xb, xl_sem, acc):
    c = pltpu.make_async_copy(x_ref, xb.at[0], xl_sem.at[0])
    c.start()
    c.wait()
    return xb[0].astype(F32)


def moe(x, ids, gates, w1, w3, w2):
    hbm = pl.BlockSpec(memory_space=pl.ANY)
    vmem = pl.BlockSpec(memory_space=pltpu.VMEM)
    dma = pltpu.SemaphoreType.DMA
    out = pl.pallas_call(
        moe_kernel,
        out_shape=(
            jax.ShapeDtypeStruct((TOK, HID), BF16),
            jax.ShapeDtypeStruct((1, 1), F32),
            jax.ShapeDtypeStruct((N_DEV, TOK, HID), BF16),
            jax.ShapeDtypeStruct((N_DEV, RET, HID), BF16),
            jax.ShapeDtypeStruct((N_DEV, RET, HID), BF16),
            jax.ShapeDtypeStruct((6, RET, HID), BF16),
        ),
        in_specs=[hbm, vmem, vmem, vmem, hbm, hbm, hbm],
        out_specs=(hbm, pl.BlockSpec(memory_space=pltpu.SMEM), hbm, hbm, hbm, hbm),
        scratch_shapes=[
            pltpu.VMEM((2, HID, FFN), BF16),
            pltpu.VMEM((2, HID, FFN), BF16),
            pltpu.VMEM((2, FFN, HID), BF16),
            pltpu.VMEM((N_LOC, 6 * CAP, HID), BF16),
            pltpu.VMEM((6 * CAP, FFN), BF16),
            pltpu.VMEM((3, TOK, HID), BF16),
            pltpu.VMEM((2, RET_PAD, HID), BF16),
            pltpu.VMEM((N_DEV, 8, TOK), F32),
            pltpu.VMEM((N_DEV, 8, TOK), F32),
            pltpu.VMEM((TOK, 2 * N_EXP), F32),
            pltpu.VMEM((TOK, HID), F32),
            dma((2, 3)), dma((3,)), dma((15,)), dma((16,)), dma((16,)), dma((16,)),
            dma((2,)), dma((16,)), dma((16,)), dma((2,)), dma((6,)), dma((6,)),
        ],
        compiler_params=pltpu.CompilerParams(
            collective_id=0, has_side_effects=True, vmem_limit_bytes=67_043_328),
        name='moe',
    )(x, ids, ids.T, gates, w1, w3, w2)
    return out[0], out[1]


def plain(x_loc, ids, gates, w_g, w_u, w_d):
    hit, picked, rank, gate = routing(ids, gates)
    code = jnp.where(picked, rank, -1.0)
    match = code.T.reshape(N_DEV, N_LOC, 1, TOK) == jnp.arange(CAP, dtype=F32)[None, None, :, None]
    send = jnp.einsum('slct,th->slch', match.astype(BF16), x_loc, preferred_element_type=F32).astype(BF16)
    recv = lax.all_to_all(send, EXPERT_AXES, 0, 0)

    def expert(args):
        rows, one, three, two = args
        h_gate = jnp.dot(rows, one, preferred_element_type=F32)
        h_up = jnp.dot(rows, three, preferred_element_type=F32)
        act = (jax.nn.silu(h_gate) * h_up).astype(BF16)
        return jnp.dot(act, two, preferred_element_type=F32).astype(BF16)

    out = lax.map(expert, (recv.transpose(1, 0, 2, 3).reshape(N_LOC, N_DEV * CAP, HID), w_g, w_u, w_d))
    back = lax.all_to_all(out.reshape(N_LOC, N_DEV, CAP, HID).transpose(1, 0, 2, 3), EXPERT_AXES, 0, 0)

    def add(acc, args):
        rows, code_e, gate_e = args
        share = jnp.where(code_e[:, None] == jnp.arange(CAP, dtype=F32)[None, :], gate_e[:, None], 0.0)
        return acc + jnp.dot(share, rows.astype(F32), precision=lax.Precision.HIGHEST), None

    total = lax.scan(add, x_loc.astype(F32), (back.reshape(N_EXP, CAP, HID), code.T, gate.T))[0]
    return total.astype(BF16)


def solution(mesh):
    def local_layer(x, ids, gates, w1, w3, w2):
        y, flag = moe(x, ids, gates, w1, w3, w2)
        return lax.cond(flag[0, 0] > 0.0, lambda: plain(x, ids, gates, w1, w3, w2), lambda: y)

    tok = P(TOKEN_AXES, None)
    w = P(EXPERT_AXES, None, None)
    return jax.shard_map(local_layer, mesh=mesh, in_specs=(tok, tok, tok, w, w, w), out_specs=tok, check_vma=False)
```

```python
import functools

import jax
import jax.numpy as jnp
from jax import lax
from jax.experimental import pallas as pl
from jax.experimental.pallas import tpu as pltpu
from jax.sharding import PartitionSpec as P

TOKEN_AXES = ('ez', 'ey', 'ex')
EXPERT_AXES = ('ex', 'ey', 'ez')
MESH = pl.DeviceIdType.MESH
BF16, F32 = jnp.bfloat16, jnp.float32

N_DEV = 16
N_LOC = 4
N_EXP = N_DEV * N_LOC
TOK = 512
HID = 2048
FFN = 1408
CAP = 96
RET = 240
RET_PAD = 256
SLOTS = N_LOC * CAP
UNITS = (1, 3, 3, 1)
FIRST = (0, 1, 4, 7)


def routing(ids, gates):
    hit = ids[:, :, None] == jnp.arange(N_EXP)[None, None, :]
    picked = jnp.any(hit, axis=1)
    gate = jnp.sum(jnp.where(hit, gates[:, :, None], 0.0), axis=1)
    below = (jnp.arange(TOK)[:, None] > jnp.arange(TOK)[None, :]).astype(BF16)
    rank = jnp.dot(below, picked.astype(BF16), preferred_element_type=F32)
    return hit, picked, rank, gate


def iota(shape, axis):
    return lax.broadcasted_iota(jnp.int32, shape, axis)


def one(mask):
    return jnp.where(mask, 1.0, 0.0)


def send_tables(ids_t, top_k):
    picked = jnp.zeros((N_EXP, TOK), F32)
    for k in range(top_k):
        picked = picked + one(ids_t[k:k + 1, :] == iota((N_EXP, TOK), 0).astype(F32))
    before = one(iota((TOK, TOK), 0) < iota((TOK, TOK), 1)).astype(BF16)
    rank = jnp.dot(picked.astype(BF16), before, preferred_element_type=F32)
    code = jnp.where(picked > 0.0, rank, -1.0)
    r, c = iota((N_EXP, N_EXP), 0), iota((N_EXP, N_EXP), 1)
    mine = one(r // N_LOC == c // N_LOC)
    lower = one((r // N_LOC == c // N_LOC) & (c < r))
    hot = picked.astype(BF16)
    cnt = jnp.sum(picked, axis=1, keepdims=True)
    off = jnp.sum(jnp.dot(lower.astype(BF16), hot, preferred_element_type=F32), axis=1, keepdims=True)
    full = jnp.sum(jnp.dot(mine.astype(BF16), hot, preferred_element_type=F32), axis=1, keepdims=True)
    over = jnp.max(one(full > RET), axis=0, keepdims=True)
    slot = iota((N_EXP, TOK), 1) - (iota((N_EXP, TOK), 0) % N_LOC) * CAP
    at = slot.astype(F32)
    used = (slot >= 0) & (slot < CAP) & (at < cnt)
    pos = jnp.where(used, off + at + 1.0, 0.0)
    return code, jnp.where(iota((N_EXP, TOK), 1) < SLOTS, pos, over)


def back_table(both, top_k):
    picked = jnp.zeros((TOK, N_EXP), F32)
    gate = jnp.zeros((TOK, N_EXP), F32)
    for k in range(top_k):
        hit = both[:, k:k + 1] == iota((TOK, N_EXP), 1).astype(F32)
        picked = picked + one(hit)
        gate = jnp.where(hit, both[:, 8 + k:9 + k], gate)
    hot = picked.astype(BF16)
    after = one(iota((TOK, TOK), 0) > iota((TOK, TOK), 1)).astype(BF16)
    rank = jnp.dot(after, hot, preferred_element_type=F32)
    r, c = iota((N_EXP, N_EXP), 0), iota((N_EXP, N_EXP), 1)
    upper = one((r // N_LOC == c // N_LOC) & (r < c)).astype(BF16)
    off = jnp.sum(jnp.dot(hot, upper, preferred_element_type=F32), axis=0, keepdims=True)
    return jnp.concatenate([jnp.where(picked > 0.0, off + rank, -1.0), gate], axis=1)


def flips(q):
    ct, i = (q + 2) // 3, (q + 2) % 3
    w1, w2, w3 = (ct % 2) * (1 - ct // 2), (1 - ct % 2) * (ct // 2), (ct % 2) * (ct // 2)
    base = ((3 - i) // 3, i % 2, i // 2)
    return tuple(w1 * f + w2 * (1 - f) + w3 for f in base)


def moe_kernel(top_k, x_ref, both_ref, w1_ref, w3_ref, w2_ref,
               y_ref, flag_ref, x_all, h_send, h_recv, h_pass,
               wb1, wb3, wb2, rows, act, xb, sb, meta, codes, comb, acc,
               w_sem, xl_sem, xs_sem, xr_sem, ms_sem, mr_sem, sl_sem, rs_sem, rr_sem, rl_sem, ps_sem, pr_sem):
    ez, ey, ex = (lax.axis_index(a) for a in TOKEN_AXES)
    core, xc = ex % 2, ex // 2
    my_tok = (ez * 2 + ey) * 4 + ex
    my_exp = (ex * 2 + ey) * 2 + ez

    def place(q, other):
        cs = core + other * (1 - 2 * core)
        return moved(q, cs, cs)

    def moved(q, cs, to_core):
        fa, fb, fc = flips(q)
        fx = fa * (1 - cs) + fb * cs
        fy = fb * (1 - cs) + fc * cs
        fz = fc * (1 - cs) + fa * cs
        pz, py, px = ez + fz * (1 - 2 * ez), ey + fy * (1 - 2 * ey), xc + fx * (1 - 2 * xc)
        return pz, py, 2 * px + to_core

    def tok_num(p):
        return (p[0] * 2 + p[1]) * 4 + p[2]

    def exp_num(p):
        return (p[2] * 2 + p[1]) * 2 + p[0]

    barrier = pltpu.get_barrier_semaphore()

    @pl.loop(1, N_DEV)
    def _(d):
        pl.semaphore_signal(barrier, inc=1, device_id=place(d // 2, d % 2), device_id_type=MESH)

    pl.semaphore_wait(barrier, N_DEV - 1)

    def x_copy(src, slot, n, dev):
        return pltpu.make_async_remote_copy(
            src_ref=src, dst_ref=x_all.at[slot], send_sem=xs_sem.at[n], recv_sem=xr_sem.at[slot],
            device_id=dev, device_id_type=MESH)

    sib = place(0, 1)
    nbr = {1: place(1, 0), 2: place(2, 0), 3: place(3, 0)}
    for n, q in enumerate((1, 2, 3)):
        x_copy(x_ref, q, n, nbr[q]).start()
    x_copy(x_ref, 8, 3, sib).start()

    def forward(q, via, to, n):
        x_copy(x_all.at[q], to, n, nbr[via]).start()

    def push(q):
        x_copy(x_all.at[q], 8 + q, 3 + q, sib).start()

    def arrived(slot):
        x_copy(x_ref, slot, 0, sib).wait_recv()

    def w_copies(e, s):
        return [pltpu.make_async_copy(w.at[e], b.at[s], w_sem.at[s, k])
                for k, (w, b) in enumerate(((w1_ref, wb1), (w3_ref, wb3), (w2_ref, wb2)))]

    for c in w_copies(0, 0):
        c.start()
    sb[:, RET:, :] = jnp.zeros((2, RET_PAD - RET, HID), BF16)

    def meta_copy(d):
        dev = place(d // 2, d % 2)
        return pltpu.make_async_remote_copy(
            src_ref=codes.at[exp_num(dev)], dst_ref=meta.at[my_tok], send_sem=ms_sem.at[d],
            recv_sem=mr_sem.at[my_tok], device_id=dev, device_id_type=MESH)

    code, pos = send_tables(both_ref[0:8, :], top_k)
    for e in range(N_DEV):
        part = slice(e * N_LOC, (e + 1) * N_LOC)
        codes[e] = jnp.concatenate([code[part], pos[part]], axis=0)
    comb[...] = back_table(both_ref[...].T, top_k)
    meta[my_tok] = codes[my_exp]

    @pl.loop(1, N_DEV)
    def _(d):
        meta_copy(d).start()

    def meta_wait(num):
        pltpu.make_async_remote_copy(
            src_ref=codes.at[0], dst_ref=meta.at[num], send_sem=ms_sem.at[0], recv_sem=mr_sem.at[num],
            device_id=sib, device_id_type=MESH).wait_recv()

    def gather(ci):
        nu, q0 = UNITS[ci], FIRST[ci]
        n = 2 * nu

        def load(g):
            src = x_all.at[q0 + g % nu + 8 * (g // nu)]
            return pltpu.make_async_copy(src, xb.at[g % 3], xl_sem.at[g % 3])

        def fetch(g):
            @pl.when(g >= nu)
            def _():
                arrived(q0 + g % nu + 8)
            load(g).start()

        if ci == 0:
            pltpu.make_async_copy(x_ref, xb.at[0], xl_sem.at[0]).start()
        else:
            fetch(0)
        fetch(1)

        @pl.loop(0, n)
        def _(g):
            @pl.when(g + 2 < n)
            def _():
                fetch(g + 2)
            d = 2 * (g % nu) + g // nu
            dev = place(q0 + d // 2, d % 2)
            num = tok_num(dev)
            if ci == 0:
                pl.when(g > 0)(lambda: meta_wait(num))
            else:
                meta_wait(num)
            code = meta[num]
            want = lax.broadcasted_iota(jnp.int32, (CAP, TOK), 0).astype(F32)
            sel = jnp.concatenate(
                [jnp.where(code[e:e + 1, :] == want, 1.0, 0.0).astype(BF16) for e in range(N_LOC)], axis=0)
            load(g).wait()
            at = pl.multiple_of(d * CAP, CAP)

            @pl.loop(0, HID // 1024)
            def _(t):
                cols = pl.ds(pl.multiple_of(t * 1024, 1024), 1024)
                got = jnp.dot(sel, xb[g % 3, :, cols], preferred_element_type=F32).astype(BF16)
                for e in range(N_LOC):
                    rows[e, pl.ds(at, CAP), cols] = got[e * CAP:(e + 1) * CAP]

    def ffn(ci, e):
        m = UNITS[ci] * 2 * CAP
        s = e % 2
        for c in w_copies(e, s):
            c.wait()
        def prefetch():
            for c in w_copies((e + 1) % N_LOC, 1 - s):
                c.start()
        if ci < 3:
            prefetch()
        else:
            pl.when(e + 1 < N_LOC)(prefetch)

        def up(at, wide):
            cols = pl.ds(at, wide)
            w = jnp.concatenate([wb1[s, :, cols], wb3[s, :, cols]], axis=1)
            h = jnp.dot(rows[e, :m, :], w, preferred_element_type=F32)
            act[:m, cols] = (jax.nn.silu(h[:, :wide]) * h[:, wide:]).astype(BF16)

        @pl.loop(0, FFN // 256)
        def _(t):
            up(pl.multiple_of(t * 256, 256), 256)

        up(FFN // 256 * 256, FFN % 256)

        @pl.loop(0, HID // 1024)
        def _(t):
            cols = pl.ds(pl.multiple_of(t * 1024, 1024), 1024)
            rows[e, :m, cols] = jnp.dot(act[:m, :], wb2[s, :, cols], preferred_element_type=F32).astype(BF16)

    def ret_copy(d):
        dev = place(d // 2, d % 2)
        return pltpu.make_async_remote_copy(
            src_ref=h_send.at[d], dst_ref=h_recv.at[my_exp], send_sem=rs_sem.at[d],
            recv_sem=rr_sem.at[my_exp], device_id=dev, device_id_type=MESH)

    def via_copy(k):
        i, c2 = k // 2, k % 2
        return pltpu.make_async_remote_copy(
            src_ref=h_send.at[2 * FIRST[2] + k], dst_ref=h_pass.at[k], send_sem=rs_sem.at[2 * FIRST[2] + k],
            recv_sem=pr_sem.at[k], device_id=place((i + 1) % 3 + 1, c2), device_id_type=MESH)

    def pass_on(k):
        i, c2 = k // 2, k % 2
        num = exp_num(moved((i + 1) % 3 + 1, core, core + c2 * (1 - 2 * core)))
        return pltpu.make_async_remote_copy(
            src_ref=h_pass.at[k], dst_ref=h_recv.at[num], send_sem=ps_sem.at[k],
            recv_sem=rr_sem.at[num], device_id=place((i + 2) % 3 + 1, 0), device_id_type=MESH)

    def stage(d):
        return pltpu.make_async_copy(sb.at[d % 2, pl.ds(0, RET)], h_send.at[d], sl_sem.at[d % 2])

    def send_back(ci):
        d0, n = 2 * FIRST[ci], 2 * UNITS[ci]

        @pl.loop(0, n)
        def _(k):
            d = d0 + k
            num = tok_num(place(d // 2, d % 2))
            pos = jnp.sum(meta[num, 4:8, :SLOTS], axis=0, keepdims=True) - 1.0
            want = lax.broadcasted_iota(jnp.int32, (RET, SLOTS), 0).astype(F32)
            sel = jnp.where(pos == want, 1.0, 0.0).astype(BF16)
            at = pl.multiple_of(k * CAP, CAP)

            @pl.loop(0, HID // 1024)
            def _(t):
                cols = pl.ds(pl.multiple_of(t * 1024, 1024), 1024)
                o = jnp.concatenate([rows[e, pl.ds(at, CAP), cols] for e in range(N_LOC)], axis=0)
                sb[d % 2, :RET, cols] = jnp.dot(sel, o, preferred_element_type=F32).astype(BF16)

            stage(d).start()

            @pl.when(k > 0)
            def _():
                stage(d - 1).wait()
                if ci == 1:
                    ret_copy(d - 1).start()
                elif ci == 2:
                    via_copy(k - 1).start()

        last = d0 + n - 1
        stage(last).wait()
        if ci == 2:
            via_copy(n - 1).start()
        elif ci < 2:
            ret_copy(last).start()

    def hand_on(first):
        @pl.loop(0, 3)
        def _(i):
            with jax.named_scope('hand'):
                via_copy(2 * i + first).wait_recv()
            pass_on(2 * i + first).start()

    def experts(ci, between=None):
        @pl.loop(0, N_LOC)
        def _(e):
            ffn(ci, e)
            if between is not None:
                pl.when(e == 2)(between)

    ns = jax.named_scope
    with ns('gather0'):
        gather(0)
    with ns('ffn0'):
        experts(0)
    with ns('send0'):
        send_back(0)
    with ns('wait_x1'):
        for q in (1, 2, 3):
            arrived(q)
            if q == 1:
                forward(1, 3, 5, 11)
            elif q == 2:
                forward(2, 1, 6, 12)
            else:
                forward(3, 2, 4, 13)
        for q in (1, 2, 3):
            push(q)
    with ns('gather1'):
        gather(1)

    def relay():
        with ns('wait_x2'):
            arrived(4)
            forward(4, 1, 7, 14)
            push(4)
            for q in (5, 6):
                arrived(q)
                push(q)

    with ns('ffn1'):
        experts(1, relay)
    with ns('send1'):
        send_back(1)
    with ns('gather2'):
        gather(2)

    def relay_last():
        with ns('wait_x3'):
            arrived(7)
            push(7)

    with ns('ffn2'):
        experts(2, relay_last)
    with ns('send2'):
        send_back(2)
    with ns('gather3'):
        gather(3)
    with ns('ffn3'):
        experts(3)
    with ns('send3'):
        send_back(3)

    acc[...] = x_to_f32(x_ref, xb, xl_sem, acc)

    def take(d):
        num = exp_num(place(d // 2, d % 2))
        return pltpu.make_async_copy(h_recv.at[num], sb.at[d % 2, pl.ds(0, RET)], rl_sem.at[d % 2])

    def came(d):
        num = exp_num(place(d // 2, d % 2))
        pltpu.make_async_remote_copy(
            src_ref=h_send.at[d], dst_ref=h_recv.at[num], send_sem=rs_sem.at[d],
            recv_sem=rr_sem.at[num], device_id=sib, device_id_type=MESH).wait_recv()

    pltpu.make_async_copy(h_send.at[0], sb.at[0, pl.ds(0, RET)], rl_sem.at[0]).start()

    def far():
        for d in (14, 15):
            ret_copy(d).start()

    @pl.loop(0, N_DEV)
    def _(d):
        pl.when(d == 2)(lambda: hand_on(0))
        pl.when(d == 5)(lambda: hand_on(1))
        pl.when(d == 8)(far)

        @pl.when(d + 1 < N_DEV)
        def _():
            with jax.named_scope('came'):
                came(d + 1)
            take(d + 1).start()
        num = exp_num(place(d // 2, d % 2))
        tab = pltpu.roll(comb[...], (2 * N_EXP - num * N_LOC) % (2 * N_EXP), 1)
        want = lax.broadcasted_iota(jnp.int32, (TOK, RET_PAD), 1).astype(F32)
        g = jnp.zeros((TOK, RET_PAD), F32)
        for e in range(N_LOC):
            g = jnp.where(tab[:, e:e + 1] == want, tab[:, N_EXP + e:N_EXP + e + 1], g)
        hi = g.astype(BF16)
        rest = g - hi.astype(F32)
        mid = rest.astype(BF16)
        lo = (rest - mid.astype(F32)).astype(BF16)
        lhs = jnp.concatenate([hi, mid, lo], axis=1)
        take(d).wait()

        @pl.loop(0, HID // 512)
        def _(t):
            cols = pl.ds(pl.multiple_of(t * 512, 512), 512)
            back = sb[d % 2, :, cols]
            acc[:, cols] += jnp.dot(lhs, jnp.concatenate([back] * 3, axis=0), preferred_element_type=F32)

    out = [pltpu.make_async_copy(xb.at[1, pl.ds(h * 256, 256)], y_ref.at[pl.ds(h * 256, 256)], xl_sem.at[h])
           for h in range(2)]
    for h in range(2):
        xb[1, h * 256:(h + 1) * 256, :] = acc[h * 256:(h + 1) * 256, :].astype(BF16)
        out[h].start()
    flag_ref[0, 0] = jnp.max(meta[:, 4, SLOTS:])

    for c in out:
        c.wait()
    for n in range(15):
        x_copy(x_ref, 0, n, sib).wait_send()

    @pl.loop(1, N_DEV)
    def _(d):
        meta_copy(d).wait_send()
        ret_copy(d).wait_send()

    @pl.loop(0, 6)
    def _(k):
        pass_on(k).wait_send()


def x_to_f32(x_ref, xb, xl_sem, acc):
    c = pltpu.make_async_copy(x_ref, xb.at[0], xl_sem.at[0])
    c.start()
    c.wait()
    return xb[0].astype(F32)


def moe(x, ids, gates, w1, w3, w2):
    pad = ((0, 8 - ids.shape[1]), (0, 0))
    both = jnp.concatenate([jnp.pad(ids.T.astype(F32), pad), jnp.pad(gates.T, pad)], axis=0)
    hbm = pl.BlockSpec(memory_space=pl.ANY)
    vmem = pl.BlockSpec(memory_space=pltpu.VMEM)
    dma = pltpu.SemaphoreType.DMA
    out = pl.pallas_call(
        functools.partial(moe_kernel, ids.shape[1]),
        out_shape=(
            jax.ShapeDtypeStruct((TOK, HID), BF16),
            jax.ShapeDtypeStruct((1, 1), F32),
            jax.ShapeDtypeStruct((N_DEV, TOK, HID), BF16),
            jax.ShapeDtypeStruct((N_DEV, RET, HID), BF16),
            jax.ShapeDtypeStruct((N_DEV, RET, HID), BF16),
            jax.ShapeDtypeStruct((6, RET, HID), BF16),
        ),
        in_specs=[hbm, vmem, hbm, hbm, hbm],
        out_specs=(hbm, pl.BlockSpec(memory_space=pltpu.SMEM), hbm, hbm, hbm, hbm),
        scratch_shapes=[
            pltpu.VMEM((2, HID, FFN), BF16),
            pltpu.VMEM((2, HID, FFN), BF16),
            pltpu.VMEM((2, FFN, HID), BF16),
            pltpu.VMEM((N_LOC, 6 * CAP, HID), BF16),
            pltpu.VMEM((6 * CAP, FFN), BF16),
            pltpu.VMEM((3, TOK, HID), BF16),
            pltpu.VMEM((2, RET_PAD, HID), BF16),
            pltpu.VMEM((N_DEV, 8, TOK), F32),
            pltpu.VMEM((N_DEV, 8, TOK), F32),
            pltpu.VMEM((TOK, 2 * N_EXP), F32),
            pltpu.VMEM((TOK, HID), F32),
            dma((2, 3)), dma((3,)), dma((15,)), dma((16,)), dma((16,)), dma((16,)),
            dma((2,)), dma((16,)), dma((16,)), dma((2,)), dma((6,)), dma((6,)),
        ],
        compiler_params=pltpu.CompilerParams(
            collective_id=0, has_side_effects=True, vmem_limit_bytes=67_043_328),
        name='moe',
    )(x, both, w1, w3, w2)
    return out[0], out[1]


def plain(x_loc, ids, gates, w_g, w_u, w_d):
    hit, picked, rank, gate = routing(ids, gates)
    code = jnp.where(picked, rank, -1.0)
    match = code.T.reshape(N_DEV, N_LOC, 1, TOK) == jnp.arange(CAP, dtype=F32)[None, None, :, None]
    send = jnp.einsum('slct,th->slch', match.astype(BF16), x_loc, preferred_element_type=F32).astype(BF16)
    recv = lax.all_to_all(send, EXPERT_AXES, 0, 0)

    def expert(args):
        rows, one, three, two = args
        h_gate = jnp.dot(rows, one, preferred_element_type=F32)
        h_up = jnp.dot(rows, three, preferred_element_type=F32)
        act = (jax.nn.silu(h_gate) * h_up).astype(BF16)
        return jnp.dot(act, two, preferred_element_type=F32).astype(BF16)

    out = lax.map(expert, (recv.transpose(1, 0, 2, 3).reshape(N_LOC, N_DEV * CAP, HID), w_g, w_u, w_d))
    back = lax.all_to_all(out.reshape(N_LOC, N_DEV, CAP, HID).transpose(1, 0, 2, 3), EXPERT_AXES, 0, 0)

    def add(acc, args):
        rows, code_e, gate_e = args
        share = jnp.where(code_e[:, None] == jnp.arange(CAP, dtype=F32)[None, :], gate_e[:, None], 0.0)
        return acc + jnp.dot(share, rows.astype(F32), precision=lax.Precision.HIGHEST), None

    total = lax.scan(add, x_loc.astype(F32), (back.reshape(N_EXP, CAP, HID), code.T, gate.T))[0]
    return total.astype(BF16)


def solution(mesh):
    def local_layer(x, ids, gates, w1, w3, w2):
        y, flag = moe(x, ids, gates, w1, w3, w2)
        return lax.cond(flag[0, 0] > 0.0, lambda: plain(x, ids, gates, w1, w3, w2), lambda: y)

    tok = P(TOKEN_AXES, None)
    w = P(EXPERT_AXES, None, None)
    return jax.shard_map(local_layer, mesh=mesh, in_specs=(tok, tok, tok, w, w, w), out_specs=tok, check_vma=False)
```

```python
import functools

import jax
import jax.numpy as jnp
from jax import lax
from jax.experimental import pallas as pl
from jax.experimental.pallas import tpu as pltpu
from jax.sharding import PartitionSpec as P

TOKEN_AXES = ('ez', 'ey', 'ex')
EXPERT_AXES = ('ex', 'ey', 'ez')
MESH = pl.DeviceIdType.MESH
BF16, F32 = jnp.bfloat16, jnp.float32

N_DEV = 16
N_LOC = 4
N_EXP = N_DEV * N_LOC
TOK = 512
HID = 2048
FFN = 1408
CAP = 96
RET = 240
RET_PAD = 256
SLOTS = N_LOC * CAP
UNITS = (1, 3, 3, 1)
FIRST = (0, 1, 4, 7)


def routing(ids, gates):
    hit = ids[:, :, None] == jnp.arange(N_EXP)[None, None, :]
    picked = jnp.any(hit, axis=1)
    gate = jnp.sum(jnp.where(hit, gates[:, :, None], 0.0), axis=1)
    below = (jnp.arange(TOK)[:, None] > jnp.arange(TOK)[None, :]).astype(BF16)
    rank = jnp.dot(below, picked.astype(BF16), preferred_element_type=F32)
    return hit, picked, rank, gate


def iota(shape, axis):
    return lax.broadcasted_iota(jnp.int32, shape, axis)


def one(mask):
    return jnp.where(mask, 1.0, 0.0)


def send_tables(ids_t, top_k):
    picked = jnp.zeros((N_EXP, TOK), F32)
    for k in range(top_k):
        picked = picked + one(ids_t[k:k + 1, :] == iota((N_EXP, TOK), 0).astype(F32))
    before = one(iota((TOK, TOK), 0) < iota((TOK, TOK), 1)).astype(BF16)
    rank = jnp.dot(picked.astype(BF16), before, preferred_element_type=F32)
    code = jnp.where(picked > 0.0, rank, -1.0)
    r, c = iota((N_EXP, N_EXP), 0), iota((N_EXP, N_EXP), 1)
    mine = one(r // N_LOC == c // N_LOC)
    lower = one((r // N_LOC == c // N_LOC) & (c < r))
    hot = picked.astype(BF16)
    cnt = jnp.sum(picked, axis=1, keepdims=True)
    off = jnp.sum(jnp.dot(lower.astype(BF16), hot, preferred_element_type=F32), axis=1, keepdims=True)
    full = jnp.sum(jnp.dot(mine.astype(BF16), hot, preferred_element_type=F32), axis=1, keepdims=True)
    over = jnp.max(one(full > RET), axis=0, keepdims=True)
    slot = iota((N_EXP, TOK), 1) - (iota((N_EXP, TOK), 0) % N_LOC) * CAP
    at = slot.astype(F32)
    used = (slot >= 0) & (slot < CAP) & (at < cnt)
    pos = jnp.where(used, off + at + 1.0, 0.0)
    return code, jnp.where(iota((N_EXP, TOK), 1) < SLOTS, pos, over)


def back_table(both, top_k):
    picked = jnp.zeros((TOK, N_EXP), F32)
    gate = jnp.zeros((TOK, N_EXP), F32)
    for k in range(top_k):
        hit = both[:, k:k + 1] == iota((TOK, N_EXP), 1).astype(F32)
        picked = picked + one(hit)
        gate = jnp.where(hit, both[:, 8 + k:9 + k], gate)
    hot = picked.astype(BF16)
    after = one(iota((TOK, TOK), 0) > iota((TOK, TOK), 1)).astype(BF16)
    rank = jnp.dot(after, hot, preferred_element_type=F32)
    r, c = iota((N_EXP, N_EXP), 0), iota((N_EXP, N_EXP), 1)
    upper = one((r // N_LOC == c // N_LOC) & (r < c)).astype(BF16)
    off = jnp.sum(jnp.dot(hot, upper, preferred_element_type=F32), axis=0, keepdims=True)
    return jnp.concatenate([jnp.where(picked > 0.0, off + rank, -1.0), gate], axis=1)


def flips(q):
    ct, i = (q + 2) // 3, (q + 2) % 3
    w1, w2, w3 = (ct % 2) * (1 - ct // 2), (1 - ct % 2) * (ct // 2), (ct % 2) * (ct // 2)
    base = ((3 - i) // 3, i % 2, i // 2)
    return tuple(w1 * f + w2 * (1 - f) + w3 for f in base)


def moe_kernel(top_k, x_ref, both_ref, w1_ref, w3_ref, w2_ref,
               y_ref, flag_ref, x_all, h_send, h_recv, h_pass,
               wb1, wb3, wb2, rows, act, xb, sb, meta, codes, comb, acc,
               w_sem, xl_sem, xs_sem, xr_sem, ms_sem, mr_sem, sl_sem, rs_sem, rr_sem, rl_sem, ps_sem, pr_sem):
    ez, ey, ex = (lax.axis_index(a) for a in TOKEN_AXES)
    core, xc = ex % 2, ex // 2
    my_tok = (ez * 2 + ey) * 4 + ex
    my_exp = (ex * 2 + ey) * 2 + ez

    def place(q, other):
        cs = core + other * (1 - 2 * core)
        return moved(q, cs, cs)

    def moved(q, cs, to_core):
        fa, fb, fc = flips(q)
        fx = fa * (1 - cs) + fb * cs
        fy = fb * (1 - cs) + fc * cs
        fz = fc * (1 - cs) + fa * cs
        pz, py, px = ez + fz * (1 - 2 * ez), ey + fy * (1 - 2 * ey), xc + fx * (1 - 2 * xc)
        return pz, py, 2 * px + to_core

    def tok_num(p):
        return (p[0] * 2 + p[1]) * 4 + p[2]

    def exp_num(p):
        return (p[2] * 2 + p[1]) * 2 + p[0]

    barrier = pltpu.get_barrier_semaphore()

    @pl.loop(1, N_DEV)
    def _(d):
        pl.semaphore_signal(barrier, inc=1, device_id=place(d // 2, d % 2), device_id_type=MESH)

    pl.semaphore_wait(barrier, N_DEV - 1)

    def x_copy(src, slot, n, dev):
        return pltpu.make_async_remote_copy(
            src_ref=src, dst_ref=x_all.at[slot], send_sem=xs_sem.at[n], recv_sem=xr_sem.at[slot],
            device_id=dev, device_id_type=MESH)

    sib = place(0, 1)
    nbr = {1: place(1, 0), 2: place(2, 0), 3: place(3, 0)}
    for n, q in enumerate((1, 2, 3)):
        x_copy(x_ref, q, n, nbr[q]).start()
    x_copy(x_ref, 8, 3, sib).start()

    def forward(q, via, to, n):
        x_copy(x_all.at[q], to, n, nbr[via]).start()

    def push(q):
        x_copy(x_all.at[q], 8 + q, 3 + q, sib).start()

    def arrived(slot):
        x_copy(x_ref, slot, 0, sib).wait_recv()

    def w_copies(e, s):
        return [pltpu.make_async_copy(w.at[e], b.at[s], w_sem.at[s, k])
                for k, (w, b) in enumerate(((w1_ref, wb1), (w3_ref, wb3), (w2_ref, wb2)))]

    for c in w_copies(0, 0):
        c.start()
    sb[:, RET:, :] = jnp.zeros((2, RET_PAD - RET, HID), BF16)

    def meta_copy(d):
        dev = place(d // 2, d % 2)
        return pltpu.make_async_remote_copy(
            src_ref=codes.at[exp_num(dev)], dst_ref=meta.at[my_tok], send_sem=ms_sem.at[d],
            recv_sem=mr_sem.at[my_tok], device_id=dev, device_id_type=MESH)

    code, pos = send_tables(both_ref[0:8, :], top_k)
    for e in range(N_DEV):
        part = slice(e * N_LOC, (e + 1) * N_LOC)
        codes[e] = jnp.concatenate([code[part], pos[part]], axis=0)
    comb[...] = back_table(both_ref[...].T, top_k)
    meta[my_tok] = codes[my_exp]

    @pl.loop(1, N_DEV)
    def _(d):
        meta_copy(d).start()

    def meta_wait(num):
        pltpu.make_async_remote_copy(
            src_ref=codes.at[0], dst_ref=meta.at[num], send_sem=ms_sem.at[0], recv_sem=mr_sem.at[num],
            device_id=sib, device_id_type=MESH).wait_recv()

    def gather(ci):
        nu, q0 = UNITS[ci], FIRST[ci]
        n = 2 * nu

        def load(g):
            src = x_all.at[q0 + g % nu + 8 * (g // nu)]
            return pltpu.make_async_copy(src, xb.at[g % 3], xl_sem.at[g % 3])

        def fetch(g):
            @pl.when(g >= nu)
            def _():
                arrived(q0 + g % nu + 8)
            load(g).start()

        if ci == 0:
            pltpu.make_async_copy(x_ref, xb.at[0], xl_sem.at[0]).start()
        else:
            fetch(0)
        fetch(1)

        @pl.loop(0, n)
        def _(g):
            @pl.when(g + 2 < n)
            def _():
                fetch(g + 2)
            d = 2 * (g % nu) + g // nu
            dev = place(q0 + d // 2, d % 2)
            num = tok_num(dev)
            if ci == 0:
                pl.when(g > 0)(lambda: meta_wait(num))
            else:
                meta_wait(num)
            code = meta[num]
            want = lax.broadcasted_iota(jnp.int32, (CAP, TOK), 0).astype(F32)
            sel = jnp.concatenate(
                [jnp.where(code[e:e + 1, :] == want, 1.0, 0.0).astype(BF16) for e in range(N_LOC)], axis=0)
            load(g).wait()
            at = pl.multiple_of(d * CAP, CAP)

            @pl.loop(0, HID // 1024)
            def _(t):
                cols = pl.ds(pl.multiple_of(t * 1024, 1024), 1024)
                got = jnp.dot(sel, xb[g % 3, :, cols], preferred_element_type=F32).astype(BF16)
                for e in range(N_LOC):
                    rows[e, pl.ds(at, CAP), cols] = got[e * CAP:(e + 1) * CAP]

    def ffn(ci, e):
        m = UNITS[ci] * 2 * CAP
        s = e % 2
        for c in w_copies(e, s):
            c.wait()
        def prefetch():
            for c in w_copies((e + 1) % N_LOC, 1 - s):
                c.start()
        if ci < 3:
            prefetch()
        else:
            pl.when(e + 1 < N_LOC)(prefetch)

        def up(at, wide):
            cols = pl.ds(at, wide)
            w = jnp.concatenate([wb1[s, :, cols], wb3[s, :, cols]], axis=1)
            h = jnp.dot(rows[e, :m, :], w, preferred_element_type=F32)
            act[:m, cols] = (jax.nn.silu(h[:, :wide]) * h[:, wide:]).astype(BF16)

        @pl.loop(0, FFN // 256)
        def _(t):
            up(pl.multiple_of(t * 256, 256), 256)

        up(FFN // 256 * 256, FFN % 256)

        @pl.loop(0, HID // 1024)
        def _(t):
            cols = pl.ds(pl.multiple_of(t * 1024, 1024), 1024)
            rows[e, :m, cols] = jnp.dot(act[:m, :], wb2[s, :, cols], preferred_element_type=F32).astype(BF16)

    def ret_copy(d):
        dev = place(d // 2, d % 2)
        return pltpu.make_async_remote_copy(
            src_ref=h_send.at[d], dst_ref=h_recv.at[my_exp], send_sem=rs_sem.at[d],
            recv_sem=rr_sem.at[my_exp], device_id=dev, device_id_type=MESH)

    def via_copy(k):
        i, c2 = k // 2, k % 2
        return pltpu.make_async_remote_copy(
            src_ref=h_send.at[2 * FIRST[2] + k], dst_ref=h_pass.at[k], send_sem=rs_sem.at[2 * FIRST[2] + k],
            recv_sem=pr_sem.at[k], device_id=place((i + 1) % 3 + 1, c2), device_id_type=MESH)

    def pass_on(k):
        i, c2 = k // 2, k % 2
        num = exp_num(moved((i + 1) % 3 + 1, core, core + c2 * (1 - 2 * core)))
        return pltpu.make_async_remote_copy(
            src_ref=h_pass.at[k], dst_ref=h_recv.at[num], send_sem=ps_sem.at[k],
            recv_sem=rr_sem.at[num], device_id=place((i + 2) % 3 + 1, 0), device_id_type=MESH)

    def stage(d):
        return pltpu.make_async_copy(sb.at[d % 2, pl.ds(0, RET)], h_send.at[d], sl_sem.at[d % 2])

    def send_back(ci):
        d0, n = 2 * FIRST[ci], 2 * UNITS[ci]

        @pl.loop(0, n)
        def _(k):
            d = d0 + k
            num = tok_num(place(d // 2, d % 2))
            pos = jnp.sum(meta[num, 4:8, :SLOTS], axis=0, keepdims=True) - 1.0
            want = lax.broadcasted_iota(jnp.int32, (RET, SLOTS), 0).astype(F32)
            sel = jnp.where(pos == want, 1.0, 0.0).astype(BF16)
            at = pl.multiple_of(k * CAP, CAP)

            @pl.loop(0, HID // 1024)
            def _(t):
                cols = pl.ds(pl.multiple_of(t * 1024, 1024), 1024)
                o = jnp.concatenate([rows[e, pl.ds(at, CAP), cols] for e in range(N_LOC)], axis=0)
                sb[d % 2, :RET, cols] = jnp.dot(sel, o, preferred_element_type=F32).astype(BF16)

            stage(d).start()

            @pl.when(k > 0)
            def _():
                stage(d - 1).wait()
                if ci == 1:
                    ret_copy(d - 1).start()
                elif ci == 2:
                    via_copy(k - 1).start()

        last = d0 + n - 1
        stage(last).wait()
        if ci == 2:
            via_copy(n - 1).start()
        elif ci < 2:
            ret_copy(last).start()

    def hand_on(first):
        @pl.loop(0, 3)
        def _(i):
            with jax.named_scope('hand'):
                via_copy(2 * i + first).wait_recv()
            pass_on(2 * i + first).start()

    def experts(ci, between=None):
        @pl.loop(0, N_LOC)
        def _(e):
            ffn(ci, e)
            if between is not None:
                pl.when(e == 2)(between)

    ns = jax.named_scope
    with ns('gather0'):
        gather(0)
    with ns('ffn0'):
        experts(0)
    with ns('send0'):
        send_back(0)
    with ns('wait_x1'):
        for q in (1, 2, 3):
            arrived(q)
            if q == 1:
                forward(1, 3, 5, 11)
            elif q == 2:
                forward(2, 1, 6, 12)
            else:
                forward(3, 2, 4, 13)
        for q in (1, 2, 3):
            push(q)
    with ns('gather1'):
        gather(1)

    def relay():
        with ns('wait_x2'):
            arrived(4)
            forward(4, 1, 7, 14)
            push(4)
            for q in (5, 6):
                arrived(q)
                push(q)

    with ns('ffn1'):
        experts(1, relay)
    with ns('send1'):
        send_back(1)
    with ns('gather2'):
        gather(2)

    def relay_last():
        with ns('wait_x3'):
            arrived(7)
            push(7)

    with ns('ffn2'):
        experts(2, relay_last)
    with ns('send2'):
        send_back(2)
    with ns('gather3'):
        gather(3)
    with ns('ffn3'):
        experts(3, lambda: hand_on(0))
    with ns('send3'):
        send_back(3)

    acc[...] = x_to_f32(x_ref, xb, xl_sem, acc)

    def take(d):
        num = exp_num(place(d // 2, d % 2))
        return pltpu.make_async_copy(h_recv.at[num], sb.at[d % 2, pl.ds(0, RET)], rl_sem.at[d % 2])

    def came(d):
        num = exp_num(place(d // 2, d % 2))
        pltpu.make_async_remote_copy(
            src_ref=h_send.at[d], dst_ref=h_recv.at[num], send_sem=rs_sem.at[d],
            recv_sem=rr_sem.at[num], device_id=sib, device_id_type=MESH).wait_recv()

    pltpu.make_async_copy(h_send.at[0], sb.at[0, pl.ds(0, RET)], rl_sem.at[0]).start()

    def far():
        hand_on(1)
        for d in (14, 15):
            ret_copy(d).start()

    @pl.loop(0, N_DEV)
    def _(d):
        pl.when(d == 3)(far)

        @pl.when(d + 1 < N_DEV)
        def _():
            with jax.named_scope('came'):
                came(d + 1)
            take(d + 1).start()
        num = exp_num(place(d // 2, d % 2))
        tab = pltpu.roll(comb[...], (2 * N_EXP - num * N_LOC) % (2 * N_EXP), 1)
        want = lax.broadcasted_iota(jnp.int32, (TOK, RET_PAD), 1).astype(F32)
        g = jnp.zeros((TOK, RET_PAD), F32)
        for e in range(N_LOC):
            g = jnp.where(tab[:, e:e + 1] == want, tab[:, N_EXP + e:N_EXP + e + 1], g)
        hi = g.astype(BF16)
        rest = g - hi.astype(F32)
        mid = rest.astype(BF16)
        lo = (rest - mid.astype(F32)).astype(BF16)
        lhs = jnp.concatenate([hi, mid, lo], axis=1)
        take(d).wait()

        @pl.loop(0, HID // 512)
        def _(t):
            cols = pl.ds(pl.multiple_of(t * 512, 512), 512)
            back = sb[d % 2, :, cols]
            acc[:, cols] += jnp.dot(lhs, jnp.concatenate([back] * 3, axis=0), preferred_element_type=F32)

    out = [pltpu.make_async_copy(xb.at[1, pl.ds(h * 256, 256)], y_ref.at[pl.ds(h * 256, 256)], xl_sem.at[h])
           for h in range(2)]
    for h in range(2):
        xb[1, h * 256:(h + 1) * 256, :] = acc[h * 256:(h + 1) * 256, :].astype(BF16)
        out[h].start()
    flag_ref[0, 0] = jnp.max(meta[:, 4, SLOTS:])

    for c in out:
        c.wait()
    for n in range(15):
        x_copy(x_ref, 0, n, sib).wait_send()

    @pl.loop(1, N_DEV)
    def _(d):
        meta_copy(d).wait_send()
        ret_copy(d).wait_send()

    @pl.loop(0, 6)
    def _(k):
        pass_on(k).wait_send()


def x_to_f32(x_ref, xb, xl_sem, acc):
    c = pltpu.make_async_copy(x_ref, xb.at[0], xl_sem.at[0])
    c.start()
    c.wait()
    return xb[0].astype(F32)


def moe(x, ids, gates, w1, w3, w2):
    pad = ((0, 8 - ids.shape[1]), (0, 0))
    both = jnp.concatenate([jnp.pad(ids.T.astype(F32), pad), jnp.pad(gates.T, pad)], axis=0)
    hbm = pl.BlockSpec(memory_space=pl.ANY)
    vmem = pl.BlockSpec(memory_space=pltpu.VMEM)
    dma = pltpu.SemaphoreType.DMA
    out = pl.pallas_call(
        functools.partial(moe_kernel, ids.shape[1]),
        out_shape=(
            jax.ShapeDtypeStruct((TOK, HID), BF16),
            jax.ShapeDtypeStruct((1, 1), F32),
            jax.ShapeDtypeStruct((N_DEV, TOK, HID), BF16),
            jax.ShapeDtypeStruct((N_DEV, RET, HID), BF16),
            jax.ShapeDtypeStruct((N_DEV, RET, HID), BF16),
            jax.ShapeDtypeStruct((6, RET, HID), BF16),
        ),
        in_specs=[hbm, vmem, hbm, hbm, hbm],
        out_specs=(hbm, pl.BlockSpec(memory_space=pltpu.SMEM), hbm, hbm, hbm, hbm),
        scratch_shapes=[
            pltpu.VMEM((2, HID, FFN), BF16),
            pltpu.VMEM((2, HID, FFN), BF16),
            pltpu.VMEM((2, FFN, HID), BF16),
            pltpu.VMEM((N_LOC, 6 * CAP, HID), BF16),
            pltpu.VMEM((6 * CAP, FFN), BF16),
            pltpu.VMEM((3, TOK, HID), BF16),
            pltpu.VMEM((2, RET_PAD, HID), BF16),
            pltpu.VMEM((N_DEV, 8, TOK), F32),
            pltpu.VMEM((N_DEV, 8, TOK), F32),
            pltpu.VMEM((TOK, 2 * N_EXP), F32),
            pltpu.VMEM((TOK, HID), F32),
            dma((2, 3)), dma((3,)), dma((15,)), dma((16,)), dma((16,)), dma((16,)),
            dma((2,)), dma((16,)), dma((16,)), dma((2,)), dma((6,)), dma((6,)),
        ],
        compiler_params=pltpu.CompilerParams(
            collective_id=0, has_side_effects=True, vmem_limit_bytes=67_043_328),
        name='moe',
    )(x, both, w1, w3, w2)
    return out[0], out[1]


def plain(x_loc, ids, gates, w_g, w_u, w_d):
    hit, picked, rank, gate = routing(ids, gates)
    code = jnp.where(picked, rank, -1.0)
    match = code.T.reshape(N_DEV, N_LOC, 1, TOK) == jnp.arange(CAP, dtype=F32)[None, None, :, None]
    send = jnp.einsum('slct,th->slch', match.astype(BF16), x_loc, preferred_element_type=F32).astype(BF16)
    recv = lax.all_to_all(send, EXPERT_AXES, 0, 0)

    def expert(args):
        rows, one, three, two = args
        h_gate = jnp.dot(rows, one, preferred_element_type=F32)
        h_up = jnp.dot(rows, three, preferred_element_type=F32)
        act = (jax.nn.silu(h_gate) * h_up).astype(BF16)
        return jnp.dot(act, two, preferred_element_type=F32).astype(BF16)

    out = lax.map(expert, (recv.transpose(1, 0, 2, 3).reshape(N_LOC, N_DEV * CAP, HID), w_g, w_u, w_d))
    back = lax.all_to_all(out.reshape(N_LOC, N_DEV, CAP, HID).transpose(1, 0, 2, 3), EXPERT_AXES, 0, 0)

    def add(acc, args):
        rows, code_e, gate_e = args
        share = jnp.where(code_e[:, None] == jnp.arange(CAP, dtype=F32)[None, :], gate_e[:, None], 0.0)
        return acc + jnp.dot(share, rows.astype(F32), precision=lax.Precision.HIGHEST), None

    total = lax.scan(add, x_loc.astype(F32), (back.reshape(N_EXP, CAP, HID), code.T, gate.T))[0]
    return total.astype(BF16)


def solution(mesh):
    def local_layer(x, ids, gates, w1, w3, w2):
        y, flag = moe(x, ids, gates, w1, w3, w2)
        return lax.cond(flag[0, 0] > 0.0, lambda: plain(x, ids, gates, w1, w3, w2), lambda: y)

    tok = P(TOKEN_AXES, None)
    w = P(EXPERT_AXES, None, None)
    return jax.shard_map(local_layer, mesh=mesh, in_specs=(tok, tok, tok, w, w, w), out_specs=tok, check_vma=False)
```
